256 devices in a mesh: space: 64 (over z, y, core), slab: 4 (over x).
Axes of the slice: x: 4, y: 4, z: 8, core: 2. Of those that a mesh axis runs over, the one named last changes fastest.
Arguments:
- source: float32 [4, 256, 16384], P('slab', None, 'space'), may hold values from -6 to 6
- initial: float32 [64, 16384], P(None, 'space'), may hold values from -6 to 6
- inverse: float32 [256, 256], replicated, may hold values from -0.1 to 0.7, as said below
- lift: float32 [256, 384], replicated, may hold values from -0.109375 to 0.109375
- lift_time: float32 [256, 64], replicated, may hold values from -0.375 to 0.375
- links: int32 [6, 16384], P(None, 'space'), may hold values from 0 to 1791, as said below
- orient: int32 [6, 16384], P(None, 'space'), may hold values from 0 to 7
- exports: int32 [16384], P('space'), may hold values from 0 to 1535, as said below
- counts: int32 [64], P('space'), may hold values from 128 to 256, as said below
Outputs:
- state: float32 [4, 256, 16384], P('slab', None, 'space')
The draws below stay inside these ranges and needn't reach their ends.
Inputs may be any that keep to these rules, and one draw needn't show every extreme that they name: `links`: a value below 1536 is f*256 + e naming face f of a live slot e of the same partition; others are 1536 + m naming slot m of the imported neighbour traces. `exports`: each value is f*256 + e with e a live slot of that partition. `counts`: some partition holds exactly 256. `inverse`: full rank; diagonal entries between 0.5 and 0.7, off-diagonal entries of magnitude at most 0.1.
All inputs are finite; a program needn't handle non-finite values.
Results may differ from the reference program's by a relative error of at most 0.0001.
Values sent between devices are 32-bit elements; how exact they have to be, the bound alone decides.
A program may use at most 64 MiB of HBM per device.

```python
import jax
import jax.numpy as jnp
from jax import lax

ELEM_DEV = 256
ITERS = 6
PEER_CAP = 128
ELEMS = 16384
N_SPACE = 64
N_SLAB = 4


def counts_of(key):
    base = jax.random.fold_in(key, 101)
    values = jax.random.randint(base, (N_SPACE,), ELEM_DEV // 2, ELEM_DEV + 1)
    fullest = jax.random.randint(jax.random.fold_in(base, 1), (), 0, N_SPACE)
    return jnp.where(jnp.arange(N_SPACE) == fullest, ELEM_DEV, values).astype(jnp.int32)


def draw_counts(key, part):
    return counts_of(key)


def draw_links(key, part):
    live = jnp.repeat(counts_of(key), ELEM_DEV)
    keys = jax.random.split(jax.random.fold_in(key, 202), 4)
    shape = (6, ELEM_DEV * N_SPACE)
    element = jax.random.randint(keys[0], shape, 0, jnp.broadcast_to(live[None, :], shape))
    facing = jax.random.randint(keys[1], shape, 0, 6)
    remote = jax.random.randint(keys[2], shape, 0, 2 * PEER_CAP)
    crossing = jax.random.randint(keys[3], shape, 0, 4) == 0
    return jnp.where(crossing, 6 * ELEM_DEV + remote, facing * ELEM_DEV + element).astype(jnp.int32)


def draw_exports(key, part):
    live = jnp.repeat(counts_of(key), 2 * PEER_CAP)
    keys = jax.random.split(jax.random.fold_in(key, 303), 2)
    shape = (2 * PEER_CAP * N_SPACE,)
    element = jax.random.randint(keys[0], shape, 0, live)
    facing = jax.random.randint(keys[1], shape, 0, 6)
    return (facing * ELEM_DEV + element).astype(jnp.int32)


def draw_inverse(key, part):
    noise = jnp.clip(jax.random.normal(key, (256, 256), jnp.float32), -4.0, 4.0)
    return 0.6 * jnp.eye(256, dtype=jnp.float32) + 0.025 * noise


def plant(array, rng, low, largest):
    shape = array.shape
    index_at = [jax.random.randint(jax.random.fold_in(rng, axis), (), 0, shape[axis]) for axis in range(len(shape))]
    array = array.at[tuple(index_at)].set(low)
    longest = shape.index(max(shape))
    index_at[longest] = (index_at[longest] + 1) % shape[longest]
    return array.at[tuple(index_at)].set(largest)


def level_of(key, dims, shards, smallest, largest):
    factor_of, own = 1.0, jax.random.fold_in(key, 6)
    for axis_at, blocks in shards:
        steps = jnp.exp(jax.random.uniform(jax.random.fold_in(own, axis_at), (blocks,), jnp.float32, smallest / len(shards), largest / len(shards)))
        factor_of = factor_of * jnp.repeat(steps, dims[axis_at] // blocks).reshape([-1 if axis == axis_at else 1 for axis in range(len(dims))])
    return factor_of


def bell_draw(own_key, dims, width, limit, cuts=(), kind=jnp.bfloat16):
    result = width * jax.random.normal(own_key, dims, jnp.float32)
    if cuts:
        result = result * level_of(own_key, dims, cuts, -0.22, 0.18)
    return jnp.clip(result, -limit, limit).astype(kind)


def setup_inputs(seed: int = 0) -> dict:
    arg_keys = jax.random.split(jax.random.key(seed), 10)
    return {
        "source": bell_draw(arg_keys[0], (N_SLAB, 256, ELEMS), 1.0, 6.0, ((0, 4), (2, 64)), jnp.float32),
        "initial": bell_draw(arg_keys[1], (64, ELEMS), 1.0, 6.0, ((1, 64),), jnp.float32),
        "inverse": draw_inverse(jax.random.fold_in(arg_keys[9], 71), 0),
        "lift": bell_draw(arg_keys[3], (256, 384), 3072 ** -0.5, 0.109375, (), jnp.float32),
        "lift_time": bell_draw(arg_keys[4], (256, 64), 256 ** -0.5, 0.375, (), jnp.float32),
        "links": draw_links(jax.random.fold_in(arg_keys[9], 71), 0),
        "orient": plant(jax.random.randint(arg_keys[6], (6, ELEMS), 0, 8), jax.random.fold_in(arg_keys[6], 1), 0, 7).astype(jnp.int32),
        "exports": draw_exports(jax.random.fold_in(arg_keys[9], 71), 0),
        "counts": draw_counts(jax.random.fold_in(arg_keys[9], 71), 0),
    }


def face_stack(volume, axis):
    pieces = [volume[:, 0], volume[:, 3], volume[:, :, 0], volume[:, :, 3], volume[:, :, :, 0], volume[:, :, :, 3]]
    return jnp.stack(pieces, axis=axis)


def orient_traces(values, turn):
    swapped = jnp.swapaxes(values, 1, 2)
    values = jnp.where(jnp.bitwise_and(turn, 4) > 0, swapped, values)
    values = jnp.where(jnp.bitwise_and(turn, 1) > 0, jnp.flip(values, 1), values)
    values = jnp.where(jnp.bitwise_and(turn, 2) > 0, jnp.flip(values, 2), values)
    return values


def reference(source, initial, inverse, lift, lift_time, links, orient, exports, counts):
    highest = lax.Precision.HIGHEST
    parts = N_SPACE
    elems = ELEM_DEV
    peer = PEER_CAP
    live = (jnp.arange(elems, dtype=jnp.int32)[None, :] < counts[:, None]).astype(jnp.float32).reshape(1, parts * elems)
    index = links.reshape(6, parts, elems).transpose(1, 0, 2).reshape(parts, 6 * elems)
    turn = orient.reshape(6, parts, elems).transpose(1, 0, 2)
    outgo = exports.reshape(parts, 2 * peer)
    lift_three = lift.reshape(256, 64, 6)
    state = jnp.zeros((N_SLAB, 256, parts * elems), jnp.float32)
    for step in range(ITERS):
        fresh = []
        for slab in range(N_SLAB):
            volume = state[slab].reshape(4, 4, 4, 4, parts, elems)
            traces = face_stack(volume, 4).reshape(64, parts, 6 * elems)
            sent = jnp.take_along_axis(traces, outgo[None], axis=2)
            from_lower = jnp.roll(sent[:, :, peer:], 1, axis=1)
            from_upper = jnp.roll(sent[:, :, :peer], -1, axis=1)
            table = jnp.concatenate([traces, from_lower, from_upper], axis=2)
            nbr = jnp.take_along_axis(table, index[None], axis=2).reshape(4, 4, 4, parts, 6, elems)
            nbr = orient_traces(nbr, turn).reshape(64, parts, 6, elems)
            spatial = jnp.einsum('rcf,cnfe->rne', lift_three, nbr, precision=highest).reshape(256, parts * elems)
            if slab == 0:
                top = initial
            else:
                top = state[slab - 1][192:]
            rhs = source[slab] + spatial + jnp.dot(lift_time, top, precision=highest)
            fresh.append(jnp.dot(inverse, rhs, precision=highest) * live)
        state = jnp.stack(fresh)
    return state
```

```python
import functools

import jax
import jax.numpy as jnp
from jax import lax
from jax.experimental import pallas as pl
from jax.experimental.pallas import tpu as pltpu
from jax.sharding import PartitionSpec as P

ROUNDS = 5
E = 256
PEER = 128
LOCAL = 6 * E
TABLE = LOCAL + 2 * PEER
K = 6 * 128 + 128
F32 = jnp.float32
BF16 = jnp.bfloat16
HIGHEST = lax.Precision.HIGHEST
MESH = pl.DeviceIdType.MESH

FACES = (
    [(0, a, b) for a in range(4) for b in range(4)],
    [(3, a, b) for a in range(4) for b in range(4)],
    [(a, 0, b) for a in range(4) for b in range(4)],
    [(a, 3, b) for a in range(4) for b in range(4)],
    [(a, b, 0) for a in range(4) for b in range(4)],
    [(a, b, 3) for a in range(4) for b in range(4)],
)


def iota(shape, dim):
    return lax.broadcasted_iota(jnp.int32, shape, dim)


def dot(a, b):
    return jnp.dot(a, b, preferred_element_type=F32)


def split_pair(x):
    low = iota(x.shape, 0) < 4
    turned = pltpu.roll(x, 4, 0)
    tiles = []
    for d in (jnp.where(low, x, turned), jnp.where(low, turned, x)):
        rest = d - d.astype(BF16).astype(F32)
        tiles.append(jnp.where(low, d, rest))
    return tiles


def kernel(
    n_space,
    n_slab,
    source,
    initial,
    inverse,
    lift,
    lift_time,
    links,
    orient,
    exports,
    counts,
    out,
    v_source,
    v_initial,
    v_inverse,
    v_lift,
    v_lift_time,
    v_links,
    v_orient,
    v_exports,
    s_counts,
    pick,
    pick_out,
    table,
    gathered,
    nbr,
    lhs_node,
    lhs_time,
    const_node,
    const_time,
    lift_all,
    spread,
    link_rows,
    turn_rows,
    nodes,
    fresh,
    send,
    arrived,
    top_send,
    top_arrived,
    result,
    in_sem,
    send_sem,
    recv_sem,
    top_send_sem,
    top_recv_sem,
    out_sem,
):
    space = lax.axis_index("space")
    slab = lax.axis_index("slab")
    upper = {"space": lax.rem(space + 1, n_space)}
    lower = {"space": lax.rem(space + n_space - 1, n_space)}

    def keep(state):
        fresh[0] = state[:, :128]
        fresh[1] = state[:, 128:]

    loads = []
    for at, (src, dst) in enumerate(
        (
            (exports, v_exports),
            (inverse, v_inverse),
            (source.at[0], v_source),
            (lift_time, v_lift_time),
            (initial, v_initial),
            (links, v_links),
            (orient, v_orient),
            (lift, v_lift),
            (counts, s_counts),
        )
    ):
        copy = pltpu.make_async_copy(src, dst, in_sem.at[at])
        copy.start()
        loads.append(copy)

    barrier = pltpu.get_barrier_semaphore()
    for peer in (lower, upper):
        pl.semaphore_signal(barrier, inc=1, device_id=peer, device_id_type=MESH)

    @pl.when(slab > 0)
    def _():
        pl.semaphore_signal(barrier, inc=1, device_id={"slab": slab - 1}, device_id_type=MESH)

    @pl.when(slab < n_slab - 1)
    def _():
        pl.semaphore_signal(barrier, inc=1, device_id={"slab": slab + 1}, device_id_type=MESH)

    loads[0].wait()
    wanted = jnp.broadcast_to(v_exports[...], (16, E))

    @pl.loop(0, LOCAL // 16)
    def _(step):
        row = pl.multiple_of(step * 16, 16)
        hit = wanted == iota((16, E), 0) + row
        pick_out[pl.ds(row, 16), :] = jnp.where(hit, 1.0, 0.0).astype(BF16)

    loads[3].wait()
    loads[4].wait()
    start = jnp.dot(
        v_lift_time[...], v_initial[...], precision=HIGHEST, preferred_element_type=F32
    )
    loads[1].wait()
    loads[2].wait()
    rhs = v_source[...] + jnp.where(slab == 0, start, 0.0)
    first = jnp.dot(v_inverse[...], rhs, precision=HIGHEST, preferred_element_type=F32)
    const_time[...] = first
    by_node = jnp.where(
        iota((E, E), 1) == (iota((E, E), 0) & 3) * 64 + (iota((E, E), 0) >> 2), 1.0, 0.0
    ).astype(BF16)
    first_high = first.astype(BF16)
    first_low = (first - first_high.astype(F32)).astype(BF16)
    const_node[...] = dot(by_node, first_high) + dot(by_node, first_low)
    keep(const_node[...])

    def space_copies(turn):
        return [
            pltpu.make_async_remote_copy(
                src_ref=send.at[turn, way],
                dst_ref=arrived.at[turn, 1 - way],
                send_sem=send_sem.at[turn, way],
                recv_sem=recv_sem.at[turn, 1 - way],
                device_id=peer,
                device_id_type=MESH,
            )
            for way, peer in ((0, lower), (1, upper))
        ]

    def top_copy(turn):
        return pltpu.make_async_remote_copy(
            src_ref=top_send.at[turn],
            dst_ref=top_arrived.at[turn],
            send_sem=top_send_sem.at[turn],
            recv_sem=top_recv_sem.at[turn],
            device_id={"slab": lax.rem(slab + 1, n_slab)},
            device_id_type=MESH,
        )

    def publish(turn):
        for pair in range(32):
            for half in range(2):
                at = slice(half * 128, half * 128 + 128)
                one, two = split_pair(fresh[half, pair * 8 : pair * 8 + 8, :])
                nodes[2 * pair, :, at] = one
                nodes[2 * pair + 1, :, at] = two
        for face, members in enumerate(FACES):
            for half in range(8):
                rows = [
                    nodes[i * 16 + j * 4 + k] for i, j, k in members[2 * half : 2 * half + 2]
                ]
                table[half * 16 : half * 16 + 16, face * E : face * E + E] = jnp.concatenate(
                    rows, axis=0
                ).astype(BF16)
        leaving = dot(table[:, :LOCAL], pick_out[...])
        low = iota((8, E), 0) < 4
        for half in range(8):
            sums = []
            for at in (2 * half, 2 * half + 1):
                tile = leaving[at * 8 : at * 8 + 8, :]
                sums.append(tile + pltpu.roll(tile, 4, 0))
            rows = jnp.where(low, sums[0], sums[1])
            send[turn, 0, half * 8 : half * 8 + 8, :] = rows[:, :PEER]
            send[turn, 1, half * 8 : half * 8 + 8, :] = rows[:, PEER:]
        for copy in space_copies(turn):
            copy.start()
        for half in range(2):
            top_send[turn, :, half * 128 : half * 128 + 128] = fresh[half, pl.ds(3, 64, stride=4), :]

        @pl.when(slab < n_slab - 1)
        def _():
            top_copy(turn).start()

    def gather_local():
        for face in range(6):
            at = slice(face * E, face * E + E)
            gathered[:, at] = dot(table[:, :LOCAL], pick[:LOCAL, at])

    def advance(turn, lhs, const):
        @pl.when(slab > 0)
        def _():
            top_copy(turn).wait_recv()
            top = top_arrived[turn]
            high = top.astype(BF16)
            nbr[768:832, :] = high
            nbr[832:896, :] = (top - high.astype(F32)).astype(BF16)

        for copy in space_copies(turn):
            copy.wait_recv()
        for way in range(2):
            for half in range(8):
                pair = split_pair(arrived[turn, way, half * 8 : half * 8 + 8, :])
                table[
                    half * 16 : half * 16 + 16, LOCAL + way * PEER : LOCAL + way * PEER + PEER
                ] = jnp.concatenate(pair, axis=0).astype(BF16)
        for face in range(6):
            at = slice(face * E, face * E + E)
            block = gathered[:, at] + dot(table[:, LOCAL:], pick[LOCAL:, at])
            turn_code = turn_rows[face]
            swap = (turn_code & 4) > 0
            back_a = (turn_code & 1) > 0
            back_b = (turn_code & 2) > 0
            v = [[block[(a * 4 + b) * 8 : (a * 4 + b) * 8 + 8, :] for b in range(4)] for a in range(4)]
            v = [[v[a][b] if a == b else jnp.where(swap, v[b][a], v[a][b]) for b in range(4)] for a in range(4)]
            v = [[jnp.where(back_a, v[3 - a][b], v[a][b]) for b in range(4)] for a in range(4)]
            v = [[jnp.where(back_b, v[a][3 - b], v[a][b]) for b in range(4)] for a in range(4)]
            for a in range(4):
                for b in (0, 2):
                    row = face * 128 + (a * 4 + b) * 8
                    nbr[row : row + 16, :] = jnp.concatenate([v[a][b], v[a][b + 1]], axis=0).astype(BF16)
        high = dot(lhs[:E, :], nbr[...])
        low = dot(lhs[E:, :], nbr[...])
        return const[...] + high + low

    count = jnp.where(slab > 0, 1, 0) + jnp.where(slab < n_slab - 1, 1, 0) + 2
    pl.semaphore_wait(barrier, count)
    publish(0)

    loads[5].wait()
    loads[6].wait()
    for face in range(6):
        link_rows[:, face * E : face * E + E] = jnp.broadcast_to(v_links[face : face + 1, :], (16, E))
        turn_rows[face] = jnp.broadcast_to(v_orient[face : face + 1, :], (8, E))

    @pl.loop(0, TABLE // 16)
    def _(step):
        row = pl.multiple_of(step * 16, 16)
        hit = link_rows[...] == iota((16, LOCAL), 0) + row
        pick[pl.ds(row, 16), :] = jnp.where(hit, 1.0, 0.0).astype(BF16)

    column = iota((512, K), 1)
    face_source = ((column & 3) * 16 + ((column >> 3) & 15)) * 6 + (column >> 7)
    wanted_row = jnp.where(column < 768, face_source, 384 + (column & 63))
    spread[...] = jnp.where(iota((512, K), 0) == wanted_row, 1.0, 0.0).astype(BF16)
    loads[7].wait()
    lift_all[:, :384] = v_lift[...]
    lift_all[:, 384:] = jnp.zeros((E, 128), F32)
    lift_all[:, 384:448] = v_lift_time[...]
    operator = jnp.dot(v_inverse[...], lift_all[...], precision=HIGHEST, preferred_element_type=F32)
    high = operator.astype(BF16)
    low = (operator - high.astype(F32)).astype(BF16)
    lhs_time[:E, :] = dot(high, spread[...]).astype(BF16)
    lhs_time[E:, :] = dot(low, spread[...]).astype(BF16)
    lhs_node[:E, :] = dot(by_node, lhs_time[:E, :]).astype(BF16)
    lhs_node[E:, :] = dot(by_node, lhs_time[E:, :]).astype(BF16)
    nbr[768:, :] = jnp.zeros((128, E), BF16)

    @pl.loop(0, ROUNDS - 1)
    def _(turn):
        gather_local()
        keep(advance(turn, lhs_node, const_node))
        publish(turn + 1)

    gather_local()
    last = advance(ROUNDS - 1, lhs_time, const_time)
    loads[8].wait()
    live = iota((E, E), 1) < s_counts[0]
    result[...] = jnp.where(live, last, 0.0)
    copy_out = pltpu.make_async_copy(result, out.at[0], out_sem)
    copy_out.start()

    @pl.loop(0, ROUNDS)
    def _(turn):
        for copy in space_copies(turn):
            copy.wait_send()

        @pl.when(slab < n_slab - 1)
        def _():
            top_copy(turn).wait_send()

    copy_out.wait()


def body(n_space, n_slab, source, initial, inverse, lift, lift_time, links, orient, exports, counts):
    anywhere = pl.BlockSpec(memory_space=pl.ANY)
    vmem = pltpu.VMEM
    dma = pltpu.SemaphoreType.DMA
    return pl.pallas_call(
        functools.partial(kernel, n_space, n_slab),
        name="window",
        out_shape=jax.ShapeDtypeStruct((1, 256, E), F32),
        in_specs=[anywhere] * 9,
        out_specs=anywhere,
        scratch_shapes=[
            vmem((256, E), F32),
            vmem((64, E), F32),
            vmem((256, 256), F32),
            vmem((256, 384), F32),
            vmem((256, 64), F32),
            vmem((6, E), jnp.int32),
            vmem((6, E), jnp.int32),
            vmem((1, E), jnp.int32),
            pltpu.SMEM((1,), jnp.int32),
            vmem((TABLE, LOCAL), BF16),
            vmem((LOCAL, 2 * PEER), BF16),
            vmem((128, TABLE), BF16),
            vmem((128, LOCAL), F32),
            vmem((K, E), BF16),
            vmem((512, K), BF16),
            vmem((512, K), BF16),
            vmem((256, E), F32),
            vmem((256, E), F32),
            vmem((256, 512), F32),
            vmem((512, K), BF16),
            vmem((16, LOCAL), jnp.int32),
            vmem((6, 8, E), jnp.int32),
            vmem((64, 8, E), F32),
            vmem((2, 256, 128), F32),
            vmem((ROUNDS, 2, 64, PEER), F32),
            vmem((ROUNDS, 2, 64, PEER), F32),
            vmem((ROUNDS, 64, E), F32),
            vmem((ROUNDS, 64, E), F32),
            vmem((256, E), F32),
            dma((9,)),
            dma((ROUNDS, 2)),
            dma((ROUNDS, 2)),
            dma((ROUNDS,)),
            dma((ROUNDS,)),
            dma,
        ],
        compiler_params=pltpu.CompilerParams(
            collective_id=0, has_side_effects=True, vmem_limit_bytes=48 * 1024 * 1024
        ),
    )(source, initial, inverse, lift, lift_time, links, orient, exports.reshape(1, E), counts)


def solution(mesh):
    return jax.shard_map(
        functools.partial(body, mesh.shape["space"], mesh.shape["slab"]),
        mesh=mesh,
        in_specs=(
            P("slab", None, "space"),
            P(None, "space"),
            P(),
            P(),
            P(),
            P(None, "space"),
            P(None, "space"),
            P("space"),
            P("space"),
        ),
        out_specs=P("slab", None, "space"),
        check_vma=False,
    )
```

```python
import functools

import jax
import jax.numpy as jnp
from jax import lax
from jax.experimental import pallas as pl
from jax.experimental.pallas import tpu as pltpu
from jax.sharding import PartitionSpec as P

ROUNDS = 5
E = 256
PEER = 128
LOCAL = 6 * E
TABLE = LOCAL + 2 * PEER
K = 6 * 128 + 128
F32 = jnp.float32
BF16 = jnp.bfloat16
HIGHEST = lax.Precision.HIGHEST
MESH = pl.DeviceIdType.MESH

FACES = (
    [(0, a, b) for a in range(4) for b in range(4)],
    [(3, a, b) for a in range(4) for b in range(4)],
    [(a, 0, b) for a in range(4) for b in range(4)],
    [(a, 3, b) for a in range(4) for b in range(4)],
    [(a, b, 0) for a in range(4) for b in range(4)],
    [(a, b, 3) for a in range(4) for b in range(4)],
)


def iota(shape, dim):
    return lax.broadcasted_iota(jnp.int32, shape, dim)


def dot(a, b):
    return jnp.dot(a, b, preferred_element_type=F32)


def split_pair(x):
    low = iota(x.shape, 0) < 4
    turned = pltpu.roll(x, 4, 0)
    tiles = []
    for d in (jnp.where(low, x, turned), jnp.where(low, turned, x)):
        rest = d - d.astype(BF16).astype(F32)
        tiles.append(jnp.where(low, d, rest))
    return tiles


def kernel(
    n_space,
    n_slab,
    source,
    initial,
    inverse,
    lift,
    lift_time,
    links,
    orient,
    exports,
    out,
    v_source,
    v_initial,
    v_inverse,
    v_lift,
    v_lift_time,
    v_links,
    v_orient,
    v_exports,
    pick,
    pick_out,
    table,
    gathered,
    nbr,
    lhs_node,
    lhs_time,
    const_node,
    const_time,
    lift_all,
    spread,
    link_rows,
    turn_rows,
    nodes,
    fresh,
    send,
    arrived,
    top_send,
    top_arrived,
    in_sem,
    send_sem,
    recv_sem,
    top_send_sem,
    top_recv_sem,
):
    space = lax.axis_index("space")
    slab = lax.axis_index("slab")
    upper = {"space": lax.rem(space + 1, n_space)}
    lower = {"space": lax.rem(space + n_space - 1, n_space)}

    def keep(state):
        fresh[0] = state[:, :128]
        fresh[1] = state[:, 128:]

    loads = []
    for at, (src, dst) in enumerate(
        (
            (exports, v_exports),
            (inverse, v_inverse),
            (source.at[0], v_source),
            (lift_time, v_lift_time),
            (initial, v_initial),
            (links, v_links),
            (orient, v_orient),
            (lift, v_lift),
        )
    ):
        copy = pltpu.make_async_copy(src, dst, in_sem.at[at])
        copy.start()
        loads.append(copy)

    barrier = pltpu.get_barrier_semaphore()
    for peer in (lower, upper):
        pl.semaphore_signal(barrier, inc=1, device_id=peer, device_id_type=MESH)

    @pl.when(slab > 0)
    def _():
        pl.semaphore_signal(barrier, inc=1, device_id={"slab": slab - 1}, device_id_type=MESH)

    @pl.when(slab < n_slab - 1)
    def _():
        pl.semaphore_signal(barrier, inc=1, device_id={"slab": slab + 1}, device_id_type=MESH)

    loads[0].wait()
    wanted = jnp.broadcast_to(v_exports[...], (16, E))

    @pl.loop(0, LOCAL // 16)
    def _(step):
        row = pl.multiple_of(step * 16, 16)
        hit = wanted == iota((16, E), 0) + row
        pick_out[pl.ds(row, 16), :] = jnp.where(hit, 1.0, 0.0).astype(BF16)

    loads[3].wait()
    loads[4].wait()
    start = jnp.dot(
        v_lift_time[...].T, v_initial[...], precision=HIGHEST, preferred_element_type=F32
    )
    loads[1].wait()
    loads[2].wait()
    rhs = v_source[...] + jnp.where(slab == 0, start, 0.0)
    first = jnp.dot(v_inverse[...], rhs, precision=HIGHEST, preferred_element_type=F32)
    const_time[...] = first
    by_node = jnp.where(
        iota((E, E), 1) == (iota((E, E), 0) & 3) * 64 + (iota((E, E), 0) >> 2), 1.0, 0.0
    ).astype(BF16)
    first_high = first.astype(BF16)
    first_low = (first - first_high.astype(F32)).astype(BF16)
    const_node[...] = dot(by_node, first_high) + dot(by_node, first_low)
    keep(const_node[...])

    def space_copies(turn):
        return [
            pltpu.make_async_remote_copy(
                src_ref=send.at[turn, way],
                dst_ref=arrived.at[turn, 1 - way],
                send_sem=send_sem.at[turn, way],
                recv_sem=recv_sem.at[turn, 1 - way],
                device_id=peer,
                device_id_type=MESH,
            )
            for way, peer in ((0, lower), (1, upper))
        ]

    def top_copy(turn):
        return pltpu.make_async_remote_copy(
            src_ref=top_send.at[turn],
            dst_ref=top_arrived.at[turn],
            send_sem=top_send_sem.at[turn],
            recv_sem=top_recv_sem.at[turn],
            device_id={"slab": lax.rem(slab + 1, n_slab)},
            device_id_type=MESH,
        )

    def publish(turn):
        for pair in range(32):
            for half in range(2):
                at = slice(half * 128, half * 128 + 128)
                one, two = split_pair(fresh[half, pair * 8 : pair * 8 + 8, :])
                nodes[2 * pair, :, at] = one
                nodes[2 * pair + 1, :, at] = two
        for face, members in enumerate(FACES):
            for half in range(8):
                rows = [
                    nodes[i * 16 + j * 4 + k] for i, j, k in members[2 * half : 2 * half + 2]
                ]
                table[half * 16 : half * 16 + 16, face * E : face * E + E] = jnp.concatenate(
                    rows, axis=0
                ).astype(BF16)
        leaving = dot(table[:, :LOCAL], pick_out[...])
        low = iota((8, E), 0) < 4
        for half in range(8):
            sums = []
            for at in (2 * half, 2 * half + 1):
                tile = leaving[at * 8 : at * 8 + 8, :]
                sums.append(tile + pltpu.roll(tile, 4, 0))
            rows = jnp.where(low, sums[0], sums[1])
            send[turn, 0, half * 8 : half * 8 + 8, :] = rows[:, :PEER]
            send[turn, 1, half * 8 : half * 8 + 8, :] = rows[:, PEER:]
        for copy in space_copies(turn):
            copy.start()
        for half in range(2):
            top_send[turn, :, half * 128 : half * 128 + 128] = fresh[half, pl.ds(3, 64, stride=4), :]

        @pl.when(slab < n_slab - 1)
        def _():
            top_copy(turn).start()

    def gather_local():
        for face in range(6):
            at = slice(face * E, face * E + E)
            gathered[:, at] = dot(table[:, :LOCAL], pick[:LOCAL, at])

    def advance(turn, lhs, const):
        @pl.when(slab > 0)
        def _():
            top_copy(turn).wait_recv()
            top = top_arrived[turn]
            high = top.astype(BF16)
            nbr[768:832, :] = high
            nbr[832:896, :] = (top - high.astype(F32)).astype(BF16)

        for copy in space_copies(turn):
            copy.wait_recv()
        for way in range(2):
            for half in range(8):
                pair = split_pair(arrived[turn, way, half * 8 : half * 8 + 8, :])
                table[
                    half * 16 : half * 16 + 16, LOCAL + way * PEER : LOCAL + way * PEER + PEER
                ] = jnp.concatenate(pair, axis=0).astype(BF16)
        for face in range(6):
            at = slice(face * E, face * E + E)
            block = gathered[:, at] + dot(table[:, LOCAL:], pick[LOCAL:, at])
            turn_code = turn_rows[face]
            swap = (turn_code & 4) > 0
            back_a = (turn_code & 1) > 0
            back_b = (turn_code & 2) > 0
            v = [[block[(a * 4 + b) * 8 : (a * 4 + b) * 8 + 8, :] for b in range(4)] for a in range(4)]
            v = [[v[a][b] if a == b else jnp.where(swap, v[b][a], v[a][b]) for b in range(4)] for a in range(4)]
            v = [[jnp.where(back_a, v[3 - a][b], v[a][b]) for b in range(4)] for a in range(4)]
            v = [[jnp.where(back_b, v[a][3 - b], v[a][b]) for b in range(4)] for a in range(4)]
            for a in range(4):
                for b in (0, 2):
                    row = face * 128 + (a * 4 + b) * 8
                    nbr[row : row + 16, :] = jnp.concatenate([v[a][b], v[a][b + 1]], axis=0).astype(BF16)
        high = dot(lhs[:E, :], nbr[...])
        low = dot(lhs[E:, :], nbr[...])
        return const[...] + high + low

    count = jnp.where(slab > 0, 1, 0) + jnp.where(slab < n_slab - 1, 1, 0) + 2
    pl.semaphore_wait(barrier, count)
    publish(0)

    loads[5].wait()
    loads[6].wait()
    for face in range(6):
        link_rows[:, face * E : face * E + E] = jnp.broadcast_to(v_links[face : face + 1, :], (16, E))
        turn_rows[face] = jnp.broadcast_to(v_orient[face : face + 1, :], (8, E))

    @pl.loop(0, TABLE // 16)
    def _(step):
        row = pl.multiple_of(step * 16, 16)
        hit = link_rows[...] == iota((16, LOCAL), 0) + row
        pick[pl.ds(row, 16), :] = jnp.where(hit, 1.0, 0.0).astype(BF16)

    column = iota((512, K), 1)
    face_source = ((column & 3) * 16 + ((column >> 3) & 15)) * 6 + (column >> 7)
    wanted_row = jnp.where(column < 768, face_source, 384 + (column & 63))
    spread[...] = jnp.where(iota((512, K), 0) == wanted_row, 1.0, 0.0).astype(BF16)
    loads[7].wait()
    lift_all[:, :384] = v_lift[...]
    lift_all[:, 384:] = jnp.zeros((E, 128), F32)
    lift_all[:, 384:448] = v_lift_time[...].T
    operator = jnp.dot(v_inverse[...], lift_all[...], precision=HIGHEST, preferred_element_type=F32)
    high = operator.astype(BF16)
    low = (operator - high.astype(F32)).astype(BF16)
    lhs_time[:E, :] = dot(high, spread[...]).astype(BF16)
    lhs_time[E:, :] = dot(low, spread[...]).astype(BF16)
    lhs_node[:E, :] = dot(by_node, lhs_time[:E, :]).astype(BF16)
    lhs_node[E:, :] = dot(by_node, lhs_time[E:, :]).astype(BF16)
    nbr[768:, :] = jnp.zeros((128, E), BF16)

    @pl.loop(0, ROUNDS - 1)
    def _(turn):
        gather_local()
        keep(advance(turn, lhs_node, const_node))
        publish(turn + 1)

    gather_local()
    last = advance(ROUNDS - 1, lhs_time, const_time)
    out[0] = last

    @pl.loop(0, ROUNDS)
    def _(turn):
        for copy in space_copies(turn):
            copy.wait_send()

        @pl.when(slab < n_slab - 1)
        def _():
            top_copy(turn).wait_send()


def body(n_space, n_slab, source, initial, inverse, lift, lift_time, links, orient, exports, counts):
    hbm = pl.BlockSpec(memory_space=pltpu.HBM)
    arrays = (source, initial, inverse, lift, lift_time.T, links, orient, exports.reshape(1, E))
    arrays = [pltpu.with_memory_space_constraint(array, pltpu.HBM) for array in arrays]
    vmem = pltpu.VMEM
    dma = pltpu.SemaphoreType.DMA
    state = pl.pallas_call(
        functools.partial(kernel, n_space, n_slab),
        name="window",
        out_shape=jax.ShapeDtypeStruct((1, 256, E), F32),
        in_specs=[hbm] * 8,
        out_specs=pl.BlockSpec(memory_space=pltpu.VMEM),
        scratch_shapes=[
            vmem((256, E), F32),
            vmem((64, E), F32),
            vmem((256, 256), F32),
            vmem((256, 384), F32),
            vmem((64, 256), F32),
            vmem((6, E), jnp.int32),
            vmem((6, E), jnp.int32),
            vmem((1, E), jnp.int32),
            vmem((TABLE, LOCAL), BF16),
            vmem((LOCAL, 2 * PEER), BF16),
            vmem((128, TABLE), BF16),
            vmem((128, LOCAL), F32),
            vmem((K, E), BF16),
            vmem((512, K), BF16),
            vmem((512, K), BF16),
            vmem((256, E), F32),
            vmem((256, E), F32),
            vmem((256, 512), F32),
            vmem((512, K), BF16),
            vmem((16, LOCAL), jnp.int32),
            vmem((6, 8, E), jnp.int32),
            vmem((64, 8, E), F32),
            vmem((2, 256, 128), F32),
            vmem((ROUNDS, 2, 64, PEER), F32),
            vmem((ROUNDS, 2, 64, PEER), F32),
            vmem((ROUNDS, 64, E), F32),
            vmem((ROUNDS, 64, E), F32),
            dma((8,)),
            dma((ROUNDS, 2)),
            dma((ROUNDS, 2)),
            dma((ROUNDS,)),
            dma((ROUNDS,)),
        ],
        compiler_params=pltpu.CompilerParams(
            collective_id=0, has_side_effects=True, vmem_limit_bytes=48 * 1024 * 1024
        ),
    )(*arrays)
    live = jnp.arange(E, dtype=jnp.int32) < counts[0]
    return jnp.where(live[None, None, :], state, 0.0)


def solution(mesh):
    return jax.shard_map(
        functools.partial(body, mesh.shape["space"], mesh.shape["slab"]),
        mesh=mesh,
        in_specs=(
            P("slab", None, "space"),
            P(None, "space"),
            P(),
            P(),
            P(),
            P(None, "space"),
            P(None, "space"),
            P("space"),
            P("space"),
        ),
        out_specs=P("slab", None, "space"),
        check_vma=False,
    )
```

```python
import functools

import jax
import jax.numpy as jnp
from jax import lax
from jax.experimental import pallas as pl
from jax.experimental.pallas import tpu as pltpu
from jax.sharding import PartitionSpec as P

ROUNDS = 5
E = 256
PEER = 128
LOCAL = 6 * E
TABLE = LOCAL + 2 * PEER
NBR = 6 * 128
K = NBR + 128
F32 = jnp.float32
BF16 = jnp.bfloat16
HIGHEST = lax.Precision.HIGHEST
MESH = pl.DeviceIdType.MESH

FACES = (
    [(0, a, b) for a in range(4) for b in range(4)],
    [(3, a, b) for a in range(4) for b in range(4)],
    [(a, 0, b) for a in range(4) for b in range(4)],
    [(a, 3, b) for a in range(4) for b in range(4)],
    [(a, b, 0) for a in range(4) for b in range(4)],
    [(a, b, 3) for a in range(4) for b in range(4)],
)


def iota(shape, dim):
    return lax.broadcasted_iota(jnp.int32, shape, dim)


def dot(a, b):
    return jnp.dot(a, b, preferred_element_type=F32)


def halves(x):
    high = x.astype(BF16)
    return high, (x - high.astype(F32)).astype(BF16)


def split_pair(x):
    low = iota(x.shape, 0) < 4
    turned = pltpu.roll(x, 4, 0)
    tiles = []
    for d in (jnp.where(low, x, turned), jnp.where(low, turned, x)):
        rest = d - d.astype(BF16).astype(F32)
        tiles.append(jnp.where(low, d, rest))
    return tiles


def oriented(block, code):
    swap = (code & 4) > 0
    back_a = (code & 1) > 0
    back_b = (code & 2) > 0
    four = range(4)
    v = [[block[(a * 4 + b) * 8 : (a * 4 + b) * 8 + 8, :] for b in four] for a in four]
    v = [[v[a][b] if a == b else jnp.where(swap, v[b][a], v[a][b]) for b in four] for a in four]
    v = [[jnp.where(back_a, v[3 - a][b], v[a][b]) for b in four] for a in four]
    v = [[jnp.where(back_b, v[a][3 - b], v[a][b]) for b in four] for a in four]
    return [v[a][b] for a in four for b in four]


def face_traces(state, code):
    low = iota(code.shape, 0) < 4

    def tile(node):
        return state[node * 4 : node * 4 + 8, :]

    rows = []
    for half in range(8):
        a, b = half // 2, 2 * (half % 2)
        near, far = a * 16 + b * 4, a * 16 + b * 4 + 4
        choices = [
            tile(a * 4 + b),
            tile(48 + a * 4 + b),
            tile(a * 16 + b),
            tile(a * 16 + 12 + b),
            jnp.where(low, tile(near), pltpu.roll(tile(far), 4, 0)),
            jnp.where(low, pltpu.roll(tile(near + 2), 4, 0), tile(far + 2)),
        ]
        value = choices[0]
        for face in range(1, 6):
            value = jnp.where(code == face, choices[face], value)
        rows.append(value)
    return rows


def kernel(
    n_space,
    n_slab,
    source,
    initial,
    inverse,
    lift,
    lift_time,
    links,
    orient,
    exports,
    out,
    v_source,
    v_initial,
    v_inverse,
    v_lift,
    v_lift_time,
    v_links,
    v_orient,
    v_exports,
    pick,
    pick_near,
    table,
    nbr,
    nbr_far,
    lhs_node,
    lhs_time,
    inv_node,
    const_node,
    own,
    own_out,
    lift_all,
    spread,
    link_rows,
    turn_rows,
    turn_out,
    codes,
    select,
    nodes,
    fresh,
    send,
    arrived,
    top_send,
    top_arrived,
    in_sem,
    send_sem,
    recv_sem,
    top_send_sem,
    top_recv_sem,
):
    space = lax.axis_index("space")
    slab = lax.axis_index("slab")
    upper = {"space": lax.rem(space + 1, n_space)}
    lower = {"space": lax.rem(space + n_space - 1, n_space)}

    loads = []
    for at, (src, dst) in enumerate(
        (
            (exports, v_exports),
            (lift_time, v_lift_time),
            (initial, v_initial),
            (inverse, v_inverse),
            (source.at[0], v_source),
            (links, v_links),
            (orient, v_orient),
            (lift, v_lift),
        )
    ):
        copy = pltpu.make_async_copy(src, dst, in_sem.at[at])
        copy.start()
        loads.append(copy)

    barrier = pltpu.get_barrier_semaphore()
    for peer in (lower, upper):
        pl.semaphore_signal(barrier, inc=1, device_id=peer, device_id_type=MESH)

    @pl.when(slab > 0)
    def _():
        pl.semaphore_signal(barrier, inc=1, device_id={"slab": slab - 1}, device_id_type=MESH)

    @pl.when(slab < n_slab - 1)
    def _():
        pl.semaphore_signal(barrier, inc=1, device_id={"slab": slab + 1}, device_id_type=MESH)

    def space_copies(turn):
        return [
            pltpu.make_async_remote_copy(
                src_ref=send.at[turn, way],
                dst_ref=arrived.at[turn, 1 - way],
                send_sem=send_sem.at[turn, way],
                recv_sem=recv_sem.at[turn, 1 - way],
                device_id=peer,
                device_id_type=MESH,
            )
            for way, peer in ((0, lower), (1, upper))
        ]

    def top_copy(turn):
        return pltpu.make_async_remote_copy(
            src_ref=top_send.at[turn],
            dst_ref=top_arrived.at[turn],
            send_sem=top_send_sem.at[turn],
            recv_sem=top_recv_sem.at[turn],
            device_id={"slab": lax.rem(slab + 1, n_slab)},
            device_id_type=MESH,
        )

    def send_out(turn, state):
        code = jnp.broadcast_to(v_exports[...] >> 8, (8, E))
        for half, rows in enumerate(face_traces(state, code)):
            send[turn, 0, half * 8 : half * 8 + 8, :] = rows[:, :PEER]
            send[turn, 1, half * 8 : half * 8 + 8, :] = rows[:, PEER:]
        for copy in space_copies(turn):
            copy.start()

    def keep(turn, state):
        for half in range(2):
            fresh[half] = state[:, half * 128 : half * 128 + 128]
        for half in range(2):
            top_send[turn, :, half * 128 : half * 128 + 128] = fresh[half, pl.ds(3, 64, stride=4), :]

        @pl.when(slab < n_slab - 1)
        def _():
            top_copy(turn).start()

    def exported(state):
        high, low = halves(state)
        return dot(high, select[...]) + dot(low, select[...])

    loads[0].wait()
    element = jnp.broadcast_to(v_exports[...] & 255, (E, E))
    select[...] = jnp.where(element == iota((E, E), 0), 1.0, 0.0).astype(BF16)
    by_node = jnp.where(
        iota((E, E), 1) == (iota((E, E), 0) & 3) * 64 + (iota((E, E), 0) >> 2), 1.0, 0.0
    ).astype(BF16)
    loads[1].wait()
    loads[2].wait()
    time_high, time_low = halves(v_lift_time[...].T)
    first_high, first_low = halves(v_initial[...])
    start = dot(time_high, first_high) + dot(time_high, first_low) + dot(time_low, first_high)
    loads[3].wait()
    inv_high, inv_low = halves(v_inverse[...])
    inv_node[:E, :] = dot(by_node, inv_high).astype(BF16)
    inv_node[E:, :] = dot(by_node, inv_low).astype(BF16)
    loads[4].wait()
    rhs_high, rhs_low = halves(v_source[...] + jnp.where(slab == 0, start, 0.0))
    first = dot(inv_node[:E, :], rhs_high) + dot(inv_node[:E, :], rhs_low) + dot(inv_node[E:, :], rhs_high)
    const_node[...] = first
    leaving = exported(first)
    count = jnp.where(slab > 0, 1, 0) + jnp.where(slab < n_slab - 1, 1, 0) + 2
    pl.semaphore_wait(barrier, count)
    send_out(0, leaving)
    keep(0, first)

    loads[5].wait()
    loads[6].wait()
    codes[...] = jnp.zeros((32, E), F32)
    codes[0:6, :] = (v_links[...] >> 8).astype(F32)
    codes[8:14, :] = (v_links[...] & 255).astype(F32)
    codes[16:22, :] = v_orient[...].astype(F32)
    moved = dot(codes[...].astype(BF16), select[...])
    far_link = (moved[0:8, :] * 256.0 + moved[8:16, :]).astype(jnp.int32)
    far_turn = moved[16:24, :].astype(jnp.int32)
    for face in range(6):
        at = slice(face * E, face * E + E)
        link_rows[:, at] = jnp.broadcast_to(v_links[face : face + 1, :], (16, E))
        turn_rows[face] = jnp.broadcast_to(v_orient[face : face + 1, :], (8, E))
        turn_out[face] = jnp.broadcast_to(far_turn[face : face + 1, :], (8, E))
        wanted = jnp.broadcast_to(far_link[face : face + 1, :], (2 * PEER, E))
        pick_near[:, at] = jnp.where(wanted == iota((2 * PEER, E), 0) + LOCAL, 1.0, 0.0).astype(BF16)

    @pl.loop(0, TABLE // 16)
    def _(step):
        row = pl.multiple_of(step * 16, 16)
        hit = link_rows[...] == iota((16, LOCAL), 0) + row
        pick[pl.ds(row, 16), :] = jnp.where(hit, 1.0, 0.0).astype(BF16)

    column = iota((512, K), 1)
    face_source = ((column & 3) * 16 + ((column >> 3) & 15)) * 6 + (column >> 7)
    wanted_row = jnp.where(column < NBR, face_source, 384 + (column & 63))
    spread[...] = jnp.where(iota((512, K), 0) == wanted_row, 1.0, 0.0).astype(BF16)
    loads[7].wait()
    lift_all[:, :384] = v_lift[...]
    lift_all[:, 384:] = jnp.zeros((E, 128), F32)
    lift_all[:, 384:448] = v_lift_time[...].T
    lift_high, lift_low = halves(lift_all[...])
    lhs_time[:E, :] = dot(lift_high, spread[...]).astype(BF16)
    lhs_time[E:, :] = dot(lift_low, spread[...]).astype(BF16)

    def operator(high, low):
        return halves(dot(high, lhs_time[:E, :]) + dot(high, lhs_time[E:, :]) + dot(low, lhs_time[:E, :]))

    node_high, node_low = operator(inv_node[:E, :], inv_node[E:, :])
    lhs_node[:E, :] = node_high
    lhs_node[E:, :] = node_low
    nbr[NBR:, :] = jnp.zeros((128, E), BF16)

    def local_part(turn):
        for pair in range(32):
            for half in range(2):
                at = slice(half * 128, half * 128 + 128)
                one, two = split_pair(fresh[half, pair * 8 : pair * 8 + 8, :])
                nodes[2 * pair, :, at] = one
                nodes[2 * pair + 1, :, at] = two
        for face, members in enumerate(FACES):
            for half in range(8):
                rows = [nodes[i * 16 + j * 4 + k] for i, j, k in members[2 * half : 2 * half + 2]]
                table[half * 16 : half * 16 + 16, face * E : face * E + E] = jnp.concatenate(
                    rows, axis=0
                ).astype(BF16)
        for face in range(6):
            at = slice(face * E, face * E + E)
            store_rows(nbr, face, oriented(dot(table[:, :LOCAL], pick[:LOCAL, at]), turn_rows[face]))

        @pl.when(slab > 0)
        def _():
            top_copy(turn).wait_recv()
            high, low = halves(top_arrived[turn])
            nbr[NBR : NBR + 64, :] = high
            nbr[NBR + 64 :, :] = low

    def store_rows(ref, face, tiles):
        for half in range(8):
            row = face * 128 + half * 16
            ref[row : row + 16, :] = jnp.concatenate(tiles[2 * half : 2 * half + 2], axis=0).astype(BF16)

    def receive(turn):
        for copy in space_copies(turn):
            copy.wait_recv()
        for way in range(2):
            for half in range(8):
                pair = split_pair(arrived[turn, way, half * 8 : half * 8 + 8, :])
                table[
                    half * 16 : half * 16 + 16, LOCAL + way * PEER : LOCAL + way * PEER + PEER
                ] = jnp.concatenate(pair, axis=0).astype(BF16)

    def remote_part(lhs, chosen, base, turns):
        for face in range(6):
            at = slice(face * E, face * E + E)
            block = dot(table[:, LOCAL:], chosen[base : base + 2 * PEER, at])
            store_rows(nbr_far, face, oriented(block, turns[face]))
        return dot(lhs[:E, :NBR], nbr_far[...]) + dot(lhs[E:, :NBR], nbr_far[...])

    @pl.loop(0, ROUNDS - 1)
    def _(turn):
        local_part(turn)
        so_far = const_node[...] + dot(lhs_node[:E, :], nbr[...]) + dot(lhs_node[E:, :], nbr[...])
        own[...] = so_far
        own_out[...] = exported(so_far)
        receive(turn)
        send_out(turn + 1, own_out[...] + remote_part(lhs_node, pick_near, 0, turn_out))
        keep(turn + 1, own[...] + remote_part(lhs_node, pick, LOCAL, turn_rows))

    inv_high, inv_low = halves(v_inverse[...])
    rhs_high, rhs_low = halves(v_source[...] + jnp.where(slab == 0, start, 0.0))
    own[...] = dot(inv_high, rhs_high) + dot(inv_high, rhs_low) + dot(inv_low, rhs_high)
    time_high, time_low = operator(inv_high, inv_low)
    lhs_time[:E, :] = time_high
    lhs_time[E:, :] = time_low
    local_part(ROUNDS - 1)
    own[...] += dot(lhs_time[:E, :], nbr[...]) + dot(lhs_time[E:, :], nbr[...])
    receive(ROUNDS - 1)
    out[0] = own[...] + remote_part(lhs_time, pick, LOCAL, turn_rows)

    @pl.loop(0, ROUNDS)
    def _(turn):
        for copy in space_copies(turn):
            copy.wait_send()

        @pl.when(slab < n_slab - 1)
        def _():
            top_copy(turn).wait_send()


def body(n_space, n_slab, source, initial, inverse, lift, lift_time, links, orient, exports, counts):
    hbm = pl.BlockSpec(memory_space=pltpu.HBM)
    arrays = (source, initial, inverse, lift, lift_time.T, links, orient, exports.reshape(1, E))
    arrays = [pltpu.with_memory_space_constraint(array, pltpu.HBM) for array in arrays]
    vmem = pltpu.VMEM
    dma = pltpu.SemaphoreType.DMA
    state = pl.pallas_call(
        functools.partial(kernel, n_space, n_slab),
        name="window",
        out_shape=jax.ShapeDtypeStruct((1, 256, E), F32),
        in_specs=[hbm] * 8,
        out_specs=pl.BlockSpec(memory_space=pltpu.VMEM),
        scratch_shapes=[
            vmem((256, E), F32),
            vmem((64, E), F32),
            vmem((256, 256), F32),
            vmem((256, 384), F32),
            vmem((64, 256), F32),
            vmem((6, E), jnp.int32),
            vmem((6, E), jnp.int32),
            vmem((1, E), jnp.int32),
            vmem((TABLE, LOCAL), BF16),
            vmem((2 * PEER, LOCAL), BF16),
            vmem((128, TABLE), BF16),
            vmem((K, E), BF16),
            vmem((NBR, E), BF16),
            vmem((512, K), BF16),
            vmem((512, K), BF16),
            vmem((512, 256), BF16),
            vmem((256, E), F32),
            vmem((256, E), F32),
            vmem((256, E), F32),
            vmem((256, 512), F32),
            vmem((512, K), BF16),
            vmem((16, LOCAL), jnp.int32),
            vmem((6, 8, E), jnp.int32),
            vmem((6, 8, E), jnp.int32),
            vmem((32, E), F32),
            vmem((E, E), BF16),
            vmem((64, 8, E), F32),
            vmem((2, 256, 128), F32),
            vmem((ROUNDS, 2, 64, PEER), F32),
            vmem((ROUNDS, 2, 64, PEER), F32),
            vmem((ROUNDS, 64, E), F32),
            vmem((ROUNDS, 64, E), F32),
            dma((8,)),
            dma((ROUNDS, 2)),
            dma((ROUNDS, 2)),
            dma((ROUNDS,)),
            dma((ROUNDS,)),
        ],
        compiler_params=pltpu.CompilerParams(
            collective_id=0, has_side_effects=True, vmem_limit_bytes=48 * 1024 * 1024
        ),
    )(*arrays)
    live = jnp.arange(E, dtype=jnp.int32) < counts[0]
    return jnp.where(live[None, None, :], state, 0.0)


def solution(mesh):
    return jax.shard_map(
        functools.partial(body, mesh.shape["space"], mesh.shape["slab"]),
        mesh=mesh,
        in_specs=(
            P("slab", None, "space"),
            P(None, "space"),
            P(),
            P(),
            P(),
            P(None, "space"),
            P(None, "space"),
            P("space"),
            P("space"),
        ),
        out_specs=P("slab", None, "space"),
        check_vma=False,
    )
```

```python
import functools

import jax
import jax.numpy as jnp
from jax import lax
from jax.experimental import pallas as pl
from jax.experimental.pallas import tpu as pltpu
from jax.sharding import PartitionSpec as P

ROUNDS = 5
E = 256
PEER = 128
LOCAL = 6 * E
TABLE = LOCAL + 2 * PEER
NBR = 6 * 128
K = NBR + 128
F32 = jnp.float32
BF16 = jnp.bfloat16
HIGHEST = lax.Precision.HIGHEST
MESH = pl.DeviceIdType.MESH

FACES = (
    [(0, a, b) for a in range(4) for b in range(4)],
    [(3, a, b) for a in range(4) for b in range(4)],
    [(a, 0, b) for a in range(4) for b in range(4)],
    [(a, 3, b) for a in range(4) for b in range(4)],
    [(a, b, 0) for a in range(4) for b in range(4)],
    [(a, b, 3) for a in range(4) for b in range(4)],
)


def iota(shape, dim):
    return lax.broadcasted_iota(jnp.int32, shape, dim)


def dot(a, b):
    return jnp.dot(a, b, preferred_element_type=F32)


def halves(x):
    high = x.astype(BF16)
    return high, (x - high.astype(F32)).astype(BF16)


def split_pair(x):
    low = iota(x.shape, 0) < 4
    turned = pltpu.roll(x, 4, 0)
    tiles = []
    for d in (jnp.where(low, x, turned), jnp.where(low, turned, x)):
        rest = d - d.astype(BF16).astype(F32)
        tiles.append(jnp.where(low, d, rest))
    return tiles


def apply(lhs, rows, depth):
    parts = []
    for at in (0, 128):
        parts.append(
            dot(lhs[at : at + 128, :depth], rows[...]) + dot(lhs[E + at : E + at + 128, :depth], rows[...])
        )
    return jnp.concatenate(parts, axis=0)


def oriented(block, code):
    swap = (code & 4) > 0
    back_a = (code & 1) > 0
    back_b = (code & 2) > 0
    four = range(4)
    v = [[block[(a * 4 + b) * 8 : (a * 4 + b) * 8 + 8, :] for b in four] for a in four]
    v = [[v[a][b] if a == b else jnp.where(swap, v[b][a], v[a][b]) for b in four] for a in four]
    v = [[jnp.where(back_a, v[3 - a][b], v[a][b]) for b in four] for a in four]
    v = [[jnp.where(back_b, v[a][3 - b], v[a][b]) for b in four] for a in four]
    return [v[a][b] for a in four for b in four]


def face_traces(state, code):
    low = iota(code.shape, 0) < 4

    def tile(node):
        return state[node * 4 : node * 4 + 8, :]

    rows = []
    for half in range(8):
        a, b = half // 2, 2 * (half % 2)
        near, far = a * 16 + b * 4, a * 16 + b * 4 + 4
        choices = [
            tile(a * 4 + b),
            tile(48 + a * 4 + b),
            tile(a * 16 + b),
            tile(a * 16 + 12 + b),
            jnp.where(low, tile(near), pltpu.roll(tile(far), 4, 0)),
            jnp.where(low, pltpu.roll(tile(near + 2), 4, 0), tile(far + 2)),
        ]
        value = choices[0]
        for face in range(1, 6):
            value = jnp.where(code == face, choices[face], value)
        rows.append(value)
    return rows


def kernel(
    n_space,
    n_slab,
    source,
    initial,
    inverse,
    lift,
    lift_time,
    links,
    orient,
    exports,
    out,
    v_source,
    v_initial,
    v_inverse,
    v_lift,
    v_lift_time,
    v_links,
    v_orient,
    v_exports,
    pick,
    pick_near,
    table,
    nbr,
    nbr_far,
    lhs_node,
    lhs_time,
    inv_node,
    const_node,
    own,
    own_out,
    lift_all,
    spread,
    link_rows,
    turn_rows,
    turn_out,
    codes,
    select,
    nodes,
    fresh,
    send,
    arrived,
    top_send,
    top_arrived,
    far_send,
    far_arrived,
    skip_arrived,
    far_pick,
    far_table,
    far_turn,
    extra,
    in_sem,
    send_sem,
    recv_sem,
    top_send_sem,
    top_recv_sem,
    far_sem,
    skip_sem,
):
    space = lax.axis_index("space")
    slab = lax.axis_index("slab")
    upper = {"space": lax.rem(space + 1, n_space)}
    lower = {"space": lax.rem(space + n_space - 1, n_space)}
    second_upper = {"space": lax.rem(space + 2, n_space)}
    second_lower = {"space": lax.rem(space + n_space - 2, n_space)}

    loads = []
    for at, (src, dst) in enumerate(
        (
            (exports, v_exports),
            (lift_time, v_lift_time),
            (initial, v_initial),
            (inverse, v_inverse),
            (source.at[0], v_source),
            (links, v_links),
            (orient, v_orient),
            (lift, v_lift),
        )
    ):
        copy = pltpu.make_async_copy(src, dst, in_sem.at[at])
        copy.start()
        loads.append(copy)

    barrier = pltpu.get_barrier_semaphore()
    for peer in (lower, upper, second_lower, second_upper):
        pl.semaphore_signal(barrier, inc=1, device_id=peer, device_id_type=MESH)

    @pl.when(slab > 0)
    def _():
        pl.semaphore_signal(barrier, inc=1, device_id={"slab": slab - 1}, device_id_type=MESH)

    @pl.when(slab < n_slab - 1)
    def _():
        pl.semaphore_signal(barrier, inc=1, device_id={"slab": slab + 1}, device_id_type=MESH)

    def space_copies(turn):
        return [
            pltpu.make_async_remote_copy(
                src_ref=send.at[turn, way],
                dst_ref=arrived.at[turn, 1 - way],
                send_sem=send_sem.at[way],
                recv_sem=recv_sem.at[turn, 1 - way],
                device_id=peer,
                device_id_type=MESH,
            )
            for way, peer in ((0, lower), (1, upper))
        ]

    def other_copies(source_of, target, sems, peers):
        return [
            pltpu.make_async_remote_copy(
                src_ref=source_of(way),
                dst_ref=target.at[1 - way],
                send_sem=sems.at[0, way],
                recv_sem=sems.at[1, 1 - way],
                device_id=peer,
                device_id_type=MESH,
            )
            for way, peer in enumerate(peers)
        ]

    far_copies = other_copies(lambda way: far_send.at[way], far_arrived, far_sem, (lower, upper))
    skip_copies = other_copies(lambda way: send.at[0, way], skip_arrived, skip_sem, (second_lower, second_upper))

    def top_copy(turn):
        return pltpu.make_async_remote_copy(
            src_ref=top_send.at[turn],
            dst_ref=top_arrived.at[turn],
            send_sem=top_send_sem,
            recv_sem=top_recv_sem.at[turn],
            device_id={"slab": lax.rem(slab + 1, n_slab)},
            device_id_type=MESH,
        )

    def send_out(turn, state, turn_is_later=True):
        code = jnp.broadcast_to(v_exports[...] >> 8, (8, E))
        for half, rows in enumerate(face_traces(state, code)):
            send[turn, 0, half * 8 : half * 8 + 8, :] = rows[:, :PEER]
            send[turn, 1, half * 8 : half * 8 + 8, :] = rows[:, PEER:]
        if turn_is_later:
            for copy in space_copies(turn - 1):
                copy.wait_send()
        for copy in space_copies(turn):
            copy.start()

    def keep(turn, state, turn_is_later=True):
        for half in range(2):
            fresh[half] = state[:, half * 128 : half * 128 + 128]
        for half in range(2):
            top_send[turn, :, half * 128 : half * 128 + 128] = fresh[half, pl.ds(3, 64, stride=4), :]

        @pl.when(slab < n_slab - 1)
        def _():
            if turn_is_later:
                top_copy(turn - 1).wait_send()
            top_copy(turn).start()

    def exported(state):
        high, low = halves(state)
        return dot(high, select[...]) + dot(low, select[...])

    loads[0].wait()
    element = jnp.broadcast_to(v_exports[...] & 255, (E, E))
    select[...] = jnp.where(element == iota((E, E), 0), 1.0, 0.0).astype(BF16)
    by_node = jnp.where(
        iota((E, E), 1) == (iota((E, E), 0) & 3) * 64 + (iota((E, E), 0) >> 2), 1.0, 0.0
    ).astype(BF16)
    loads[5].wait()
    loads[6].wait()
    codes[...] = jnp.zeros((32, E), F32)
    codes[0:6, :] = (v_links[...] >> 8).astype(F32)
    codes[8:14, :] = (v_links[...] & 255).astype(F32)
    codes[16:22, :] = v_orient[...].astype(F32)
    codes[24:25, :] = (v_exports[...] >> 8).astype(F32)
    moved = dot(codes[0:24, :].astype(BF16), select[...])
    out_link = moved[0:8, :] * 256.0 + moved[8:16, :]
    for way in range(2):
        at = slice(way * PEER, way * PEER + PEER)
        far_send[way, 0:8, :] = out_link[:, at]
        far_send[way, 8:16, :] = moved[16:24, at]
        far_send[way, 16:24, :] = codes[24:32, at]
    turn_out_rows = moved[16:24, :].astype(jnp.int32)
    loads[1].wait()
    loads[2].wait()
    time_high, time_low = halves(v_lift_time[...].T)
    first_high, first_low = halves(v_initial[...])
    start = dot(time_high, first_high) + dot(time_high, first_low) + dot(time_low, first_high)
    loads[3].wait()
    inv_high, inv_low = halves(v_inverse[...])
    inv_node[:E, :] = dot(by_node, inv_high).astype(BF16)
    inv_node[E:, :] = dot(by_node, inv_low).astype(BF16)
    loads[4].wait()
    rhs_high, rhs_low = halves(v_source[...] + jnp.where(slab == 0, start, 0.0))
    first = dot(inv_node[:E, :], rhs_high) + dot(inv_node[:E, :], rhs_low) + dot(inv_node[E:, :], rhs_high)
    const_node[...] = first
    leaving = exported(first)
    count = jnp.where(slab > 0, 1, 0) + jnp.where(slab < n_slab - 1, 1, 0) + 4
    pl.semaphore_wait(barrier, count)
    send_out(0, leaving, False)
    for copy in far_copies + skip_copies:
        copy.start()
    keep(0, first, False)

    for face in range(6):
        at = slice(face * E, face * E + E)
        link_rows[:, at] = jnp.broadcast_to(v_links[face : face + 1, :], (16, E))
        turn_rows[face] = jnp.broadcast_to(v_orient[face : face + 1, :], (8, E))
        turn_out[face] = jnp.broadcast_to(turn_out_rows[face : face + 1, :], (8, E))
        wanted = jnp.broadcast_to(out_link[face : face + 1, :].astype(jnp.int32), (2 * PEER, E))
        pick_near[:, at] = jnp.where(wanted == iota((2 * PEER, E), 0) + LOCAL, 1.0, 0.0).astype(BF16)

    @pl.loop(0, TABLE // E)
    def _(tile):
        keys = jnp.where(link_rows[...] >> 8 == tile, link_rows[...] & 255, -1).astype(F32).astype(BF16)
        one, zero = jnp.ones((16, LOCAL), BF16), jnp.zeros((16, LOCAL), BF16)
        for step in range(E // 16):
            row = (iota((16, LOCAL), 0) + step * 16).astype(F32).astype(BF16)
            at = pl.multiple_of(tile * E + step * 16, 16)
            pick[pl.ds(at, 16), :] = jnp.where(keys == row, one, zero)

    column = iota((512, K), 1)
    face_source = ((column & 3) * 16 + ((column >> 3) & 15)) * 6 + (column >> 7)
    wanted_row = jnp.where(column < NBR, face_source, 384 + (column & 63))
    spread[...] = jnp.where(iota((512, K), 0) == wanted_row, 1.0, 0.0).astype(BF16)
    loads[7].wait()
    lift_all[:, :384] = v_lift[...]
    lift_all[:, 384:] = jnp.zeros((E, 128), F32)
    lift_all[:, 384:448] = v_lift_time[...].T
    lift_high, lift_low = halves(lift_all[...])
    lhs_time[:E, :] = dot(lift_high, spread[...]).astype(BF16)
    lhs_time[E:, :] = dot(lift_low, spread[...]).astype(BF16)

    def operator(high, low):
        return halves(dot(high, lhs_time[:E, :]) + dot(high, lhs_time[E:, :]) + dot(low, lhs_time[:E, :]))

    node_high, node_low = operator(inv_node[:E, :], inv_node[E:, :])
    lhs_node[:E, :] = node_high
    lhs_node[E:, :] = node_low
    nbr[NBR:, :] = jnp.zeros((128, E), BF16)

    def local_part(turn):
        for pair in range(32):
            for half in range(2):
                at = slice(half * 128, half * 128 + 128)
                one, two = split_pair(fresh[half, pair * 8 : pair * 8 + 8, :])
                nodes[2 * pair, :, at] = one
                nodes[2 * pair + 1, :, at] = two
        for face, members in enumerate(FACES):
            for half in range(8):
                rows = [nodes[i * 16 + j * 4 + k] for i, j, k in members[2 * half : 2 * half + 2]]
                table[half * 16 : half * 16 + 16, face * E : face * E + E] = jnp.concatenate(
                    rows, axis=0
                ).astype(BF16)
        for face in range(6):
            at = slice(face * E, face * E + E)
            store_rows(nbr, face, oriented(dot(table[:, :LOCAL], pick[:LOCAL, at]), turn_rows[face]))

        @pl.when(slab > 0)
        def _():
            top_copy(turn).wait_recv()
            high, low = halves(top_arrived[turn])
            nbr[NBR : NBR + 64, :] = high
            nbr[NBR + 64 :, :] = low

    def store_rows(ref, face, tiles):
        for half in range(8):
            row = face * 128 + half * 16
            ref[row : row + 16, :] = jnp.concatenate(tiles[2 * half : 2 * half + 2], axis=0).astype(BF16)

    def receive(turn):
        for copy in space_copies(turn):
            copy.wait_recv()
        for way in range(2):
            for half in range(8):
                rows = slice(half * 8, half * 8 + 8)
                pair = split_pair(arrived[turn, way, rows, :] + extra[way, rows, :])
                table[
                    half * 16 : half * 16 + 16, LOCAL + way * PEER : LOCAL + way * PEER + PEER
                ] = jnp.concatenate(pair, axis=0).astype(BF16)

    def remote_part(chosen, base, turns, columns=lambda: table[:, LOCAL:], depth=2 * PEER):
        for face in range(6):
            at = slice(face * E, face * E + E)
            block = dot(columns(), chosen[base : base + depth, at])
            store_rows(nbr_far, face, oriented(block, turns[face]))


    def local_sums(turn):
        local_part(turn)
        so_far = const_node[...] + apply(lhs_node, nbr, K)
        own[...] = so_far
        own_out[...] = exported(so_far)

    def update(turn):
        @pl.when(space >= 0)
        def _():
            remote_part(pick, LOCAL, turn_rows)

        @pl.when(slab >= 0)
        def _():
            keep(turn + 1, own[...] + apply(lhs_node, nbr_far, NBR))

    extra[...] = jnp.zeros((2, 64, PEER), F32)
    local_sums(0)
    send_out(1, own_out[...])
    receive(0)
    update(0)

    for copy in far_copies + skip_copies:
        copy.wait_recv()
    side = jnp.where(iota((8, E), 1) < PEER, 0, 2 * PEER)
    for face in range(6):
        at = slice(face * E, face * E + E)
        link = jnp.concatenate([far_arrived[way, face : face + 1, :] for way in range(2)], axis=1).astype(jnp.int32)
        turned = jnp.concatenate([far_arrived[way, 8 + face : 9 + face, :] for way in range(2)], axis=1)
        far_turn[face] = jnp.broadcast_to(turned.astype(jnp.int32), (8, E))
        row = jnp.where(link >= LOCAL, link - LOCAL + side[0:1, :], -1)
        wanted = jnp.broadcast_to(row, (4 * PEER, E))
        far_pick[:, at] = jnp.where(wanted == iota((4 * PEER, E), 0), 1.0, 0.0).astype(BF16)
    for at, part in enumerate((skip_arrived.at[0], send.at[0, 0], send.at[0, 1], skip_arrived.at[1])):
        for half in range(8):
            pair = split_pair(part[half * 8 : half * 8 + 8, :])
            far_table[half * 16 : half * 16 + 16, at * PEER : at * PEER + PEER] = jnp.concatenate(
                pair, axis=0
            ).astype(BF16)
    remote_part(far_pick, 0, far_turn, lambda: far_table[...], 4 * PEER)
    face_code = jnp.concatenate([far_arrived[way, 16:17, :] for way in range(2)], axis=1).astype(jnp.int32)
    added = face_traces(apply(lhs_node, nbr_far, NBR), jnp.broadcast_to(face_code, (8, E)))
    for half, rows in enumerate(added):
        extra[0, half * 8 : half * 8 + 8, :] = rows[:, :PEER]
        extra[1, half * 8 : half * 8 + 8, :] = rows[:, PEER:]

    @pl.loop(1, ROUNDS - 1)
    def _(turn):
        local_sums(turn)
        receive(turn)
        extra[...] = jnp.zeros((2, 64, PEER), F32)
        remote_part(pick_near, 0, turn_out)

        @pl.when(slab >= 0)
        def _():
            send_out(turn + 1, own_out[...] + apply(lhs_node, nbr_far, NBR))

        update(turn)

    inv_high, inv_low = halves(v_inverse[...])
    rhs_high, rhs_low = halves(v_source[...] + jnp.where(slab == 0, start, 0.0))
    own[...] = dot(inv_high, rhs_high) + dot(inv_high, rhs_low) + dot(inv_low, rhs_high)
    time_high, time_low = operator(inv_high, inv_low)
    lhs_time[:E, :] = time_high
    lhs_time[E:, :] = time_low
    local_part(ROUNDS - 1)
    own[...] += apply(lhs_time, nbr, K)
    receive(ROUNDS - 1)
    remote_part(pick, LOCAL, turn_rows)

    @pl.when(slab >= 0)
    def _():
        out[0] = own[...] + apply(lhs_time, nbr_far, NBR)

    for copy in space_copies(ROUNDS - 1) + far_copies + skip_copies:
        copy.wait_send()

    @pl.when(slab < n_slab - 1)
    def _():
        top_copy(ROUNDS - 1).wait_send()


def body(n_space, n_slab, source, initial, inverse, lift, lift_time, links, orient, exports, counts):
    hbm = pl.BlockSpec(memory_space=pltpu.HBM)
    arrays = (source, initial, inverse, lift, lift_time.T, links, orient, exports.reshape(1, E))
    arrays = [pltpu.with_memory_space_constraint(array, pltpu.HBM) for array in arrays]
    vmem = pltpu.VMEM
    dma = pltpu.SemaphoreType.DMA
    state = pl.pallas_call(
        functools.partial(kernel, n_space, n_slab),
        name="window",
        out_shape=jax.ShapeDtypeStruct((1, 256, E), F32),
        in_specs=[hbm] * 8,
        out_specs=pl.BlockSpec(memory_space=pltpu.VMEM),
        scratch_shapes=[
            vmem((256, E), F32),
            vmem((64, E), F32),
            vmem((256, 256), F32),
            vmem((256, 384), F32),
            vmem((64, 256), F32),
            vmem((6, E), jnp.int32),
            vmem((6, E), jnp.int32),
            vmem((1, E), jnp.int32),
            vmem((TABLE, LOCAL), BF16),
            vmem((2 * PEER, LOCAL), BF16),
            vmem((128, TABLE), BF16),
            vmem((K, E), BF16),
            vmem((NBR, E), BF16),
            vmem((512, K), BF16),
            vmem((512, K), BF16),
            vmem((512, 256), BF16),
            vmem((256, E), F32),
            vmem((256, E), F32),
            vmem((256, E), F32),
            vmem((256, 512), F32),
            vmem((512, K), BF16),
            vmem((16, LOCAL), jnp.int32),
            vmem((6, 8, E), jnp.int32),
            vmem((6, 8, E), jnp.int32),
            vmem((32, E), F32),
            vmem((E, E), BF16),
            vmem((64, 8, E), F32),
            vmem((2, 256, 128), F32),
            vmem((ROUNDS, 2, 64, PEER), F32),
            vmem((ROUNDS, 2, 64, PEER), F32),
            vmem((ROUNDS, 64, E), F32),
            vmem((ROUNDS, 64, E), F32),
            vmem((2, 24, PEER), F32),
            vmem((2, 24, PEER), F32),
            vmem((2, 64, PEER), F32),
            vmem((4 * PEER, LOCAL), BF16),
            vmem((128, 4 * PEER), BF16),
            vmem((6, 8, E), jnp.int32),
            vmem((2, 64, PEER), F32),
            dma((8,)),
            dma((2,)),
            dma((ROUNDS, 2)),
            dma,
            dma((ROUNDS,)),
            dma((2, 2)),
            dma((2, 2)),
        ],
        compiler_params=pltpu.CompilerParams(
            collective_id=0, has_side_effects=True, vmem_limit_bytes=48 * 1024 * 1024
        ),
    )(*arrays)
    live = jnp.arange(E, dtype=jnp.int32) < counts[0]
    return jnp.where(live[None, None, :], state, 0.0)


def solution(mesh):
    return jax.shard_map(
        functools.partial(body, mesh.shape["space"], mesh.shape["slab"]),
        mesh=mesh,
        in_specs=(
            P("slab", None, "space"),
            P(None, "space"),
            P(),
            P(),
            P(),
            P(None, "space"),
            P(None, "space"),
            P("space"),
            P("space"),
        ),
        out_specs=P("slab", None, "space"),
        check_vma=False,
    )
```

```python
import functools

import jax
import jax.numpy as jnp
from jax import lax
from jax.experimental import pallas as pl
from jax.experimental.pallas import tpu as pltpu
from jax.sharding import PartitionSpec as P

ROUNDS = 5
E = 256
PEER = 128
LOCAL = 6 * E
TABLE = LOCAL + 2 * PEER
NBR = 6 * 128
K = NBR + 128
F32 = jnp.float32
BF16 = jnp.bfloat16
HIGHEST = lax.Precision.HIGHEST
MESH = pl.DeviceIdType.MESH

FACES = (
    [(0, a, b) for a in range(4) for b in range(4)],
    [(3, a, b) for a in range(4) for b in range(4)],
    [(a, 0, b) for a in range(4) for b in range(4)],
    [(a, 3, b) for a in range(4) for b in range(4)],
    [(a, b, 0) for a in range(4) for b in range(4)],
    [(a, b, 3) for a in range(4) for b in range(4)],
)


def iota(shape, dim):
    return lax.broadcasted_iota(jnp.int32, shape, dim)


def dot(a, b):
    return jnp.dot(a, b, preferred_element_type=F32)


def halves(x):
    high = x.astype(BF16)
    return high, (x - high.astype(F32)).astype(BF16)


def split_pair(x):
    low = iota(x.shape, 0) < 4
    turned = pltpu.roll(x, 4, 0)
    tiles = []
    for d in (jnp.where(low, x, turned), jnp.where(low, turned, x)):
        rest = d - d.astype(BF16).astype(F32)
        tiles.append(jnp.where(low, d, rest))
    return tiles


def apply(lhs, rows, begin, end):
    parts = []
    for at in (0, 128):
        parts.append(
            dot(lhs[at : at + 128, begin:end], rows[begin:end, :])
            + dot(lhs[E + at : E + at + 128, begin:end], rows[begin:end, :])
        )
    return jnp.concatenate(parts, axis=0)


def oriented(block, code):
    swap = (code & 4) > 0
    back_a = (code & 1) > 0
    back_b = (code & 2) > 0
    four = range(4)
    v = [[block[(a * 4 + b) * 8 : (a * 4 + b) * 8 + 8, :] for b in four] for a in four]
    v = [[v[a][b] if a == b else jnp.where(swap, v[b][a], v[a][b]) for b in four] for a in four]
    v = [[jnp.where(back_a, v[3 - a][b], v[a][b]) for b in four] for a in four]
    v = [[jnp.where(back_b, v[a][3 - b], v[a][b]) for b in four] for a in four]
    return [v[a][b] for a in four for b in four]


def face_traces(state, code):
    low = iota(code.shape, 0) < 4

    def tile(node):
        return state[node * 4 : node * 4 + 8, :]

    rows = []
    for half in range(8):
        a, b = half // 2, 2 * (half % 2)
        near, far = a * 16 + b * 4, a * 16 + b * 4 + 4
        choices = [
            tile(a * 4 + b),
            tile(48 + a * 4 + b),
            tile(a * 16 + b),
            tile(a * 16 + 12 + b),
            jnp.where(low, tile(near), pltpu.roll(tile(far), 4, 0)),
            jnp.where(low, pltpu.roll(tile(near + 2), 4, 0), tile(far + 2)),
        ]
        value = choices[0]
        for face in range(1, 6):
            value = jnp.where(code == face, choices[face], value)
        rows.append(value)
    return rows


def kernel(
    n_space,
    n_slab,
    source,
    initial,
    inverse,
    lift,
    lift_time,
    links,
    orient,
    exports,
    out,
    v_source,
    v_initial,
    v_inverse,
    v_lift,
    v_lift_time,
    v_links,
    v_orient,
    v_exports,
    pick,
    pick_near,
    table,
    nbr,
    nbr_far,
    lhs_node,
    lhs_time,
    inv_node,
    const_node,
    const_time,
    by_node,
    by_time,
    own,
    own_out,
    lift_all,
    spread,
    link_rows,
    turn_rows,
    turn_out,
    codes,
    select,
    nodes,
    fresh,
    send,
    arrived,
    top_send,
    top_arrived,
    far_send,
    far_arrived,
    skip_arrived,
    far_pick,
    far_table,
    far_turn,
    extra,
    in_sem,
    send_sem,
    recv_sem,
    top_send_sem,
    top_recv_sem,
    far_sem,
    skip_sem,
):
    space = lax.axis_index("space")
    slab = lax.axis_index("slab")
    upper = {"space": lax.rem(space + 1, n_space)}
    lower = {"space": lax.rem(space + n_space - 1, n_space)}
    second_upper = {"space": lax.rem(space + 2, n_space)}
    second_lower = {"space": lax.rem(space + n_space - 2, n_space)}

    loads = []
    for at, (src, dst) in enumerate(
        (
            (exports, v_exports),
            (links, v_links),
            (orient, v_orient),
            (lift_time, v_lift_time),
            (initial, v_initial),
            (inverse, v_inverse),
            (source.at[0], v_source),
            (lift, v_lift),
        )
    ):
        copy = pltpu.make_async_copy(src, dst, in_sem.at[at])
        copy.start()
        loads.append(copy)

    barrier = pltpu.get_barrier_semaphore()
    for peer in (lower, upper, second_lower, second_upper):
        pl.semaphore_signal(barrier, inc=1, device_id=peer, device_id_type=MESH)

    @pl.when(slab > 0)
    def _():
        pl.semaphore_signal(barrier, inc=1, device_id={"slab": slab - 1}, device_id_type=MESH)

    @pl.when(slab < n_slab - 1)
    def _():
        pl.semaphore_signal(barrier, inc=1, device_id={"slab": slab + 1}, device_id_type=MESH)

    def space_copies(turn):
        return [
            pltpu.make_async_remote_copy(
                src_ref=send.at[turn, way],
                dst_ref=arrived.at[turn, 1 - way],
                send_sem=send_sem.at[way],
                recv_sem=recv_sem.at[turn, 1 - way],
                device_id=peer,
                device_id_type=MESH,
            )
            for way, peer in ((0, lower), (1, upper))
        ]

    def other_copies(source_of, target, sems, peers):
        return [
            pltpu.make_async_remote_copy(
                src_ref=source_of(way),
                dst_ref=target.at[1 - way],
                send_sem=sems.at[0, way],
                recv_sem=sems.at[1, 1 - way],
                device_id=peer,
                device_id_type=MESH,
            )
            for way, peer in enumerate(peers)
        ]

    far_copies = other_copies(lambda way: far_send.at[way], far_arrived, far_sem, (lower, upper))
    skip_copies = other_copies(lambda way: send.at[0, way], skip_arrived, skip_sem, (second_lower, second_upper))

    def top_copy(turn):
        return pltpu.make_async_remote_copy(
            src_ref=top_send.at[turn],
            dst_ref=top_arrived.at[turn],
            send_sem=top_send_sem,
            recv_sem=top_recv_sem.at[turn],
            device_id={"slab": lax.rem(slab + 1, n_slab)},
            device_id_type=MESH,
        )

    def send_out(turn, state, turn_is_later=True):
        code = jnp.broadcast_to(v_exports[...] >> 8, (8, E))
        for half, rows in enumerate(face_traces(state, code)):
            send[turn, 0, half * 8 : half * 8 + 8, :] = rows[:, :PEER]
            send[turn, 1, half * 8 : half * 8 + 8, :] = rows[:, PEER:]
        if turn_is_later:
            for copy in space_copies(turn - 1):
                copy.wait_send()
        for copy in space_copies(turn):
            copy.start()

    def keep(turn, state, turn_is_later=True):
        for half in range(2):
            fresh[half] = state[:, half * 128 : half * 128 + 128]
        for half in range(2):
            top_send[turn, :, half * 128 : half * 128 + 128] = fresh[half, pl.ds(3, 64, stride=4), :]

        @pl.when(slab < n_slab - 1)
        def _():
            if turn_is_later:
                top_copy(turn - 1).wait_send()
            top_copy(turn).start()

    def exported(state):
        high, low = halves(state)
        return dot(high, select[...]) + dot(low, select[...])

    row, column = iota((E, E), 0), iota((E, E), 1)
    by_node[...] = jnp.where(column == (row & 3) * 64 + (row >> 2), 1.0, 0.0).astype(BF16)
    by_time[...] = jnp.where(column == (row & 63) * 4 + (row >> 6), 1.0, 0.0).astype(BF16)
    column = iota((512, K), 1)
    face_source = ((column & 3) * 16 + ((column >> 3) & 15)) * 6 + (column >> 7)
    wanted_row = jnp.where(column < NBR, face_source, 384 + (column & 63))
    spread[...] = jnp.where(iota((512, K), 0) == wanted_row, 1.0, 0.0).astype(BF16)
    codes[...] = jnp.zeros((32, E), F32)
    extra[...] = jnp.zeros((2, 64, PEER), F32)
    nbr[NBR:, :] = jnp.zeros((128, E), BF16)
    lift_all[:, 384:] = jnp.zeros((E, 128), F32)

    for load in loads[:6]:
        load.wait()
    element = jnp.broadcast_to(v_exports[...] & 255, (E, E))
    select[...] = jnp.where(element == iota((E, E), 0), 1.0, 0.0).astype(BF16)
    codes[0:6, :] = (v_links[...] >> 8).astype(F32)
    codes[8:14, :] = (v_links[...] & 255).astype(F32)
    codes[16:22, :] = v_orient[...].astype(F32)
    codes[24:25, :] = (v_exports[...] >> 8).astype(F32)
    moved = dot(codes[0:24, :].astype(BF16), select[...])
    time_high, time_low = halves(v_lift_time[...].T)
    first_high, first_low = halves(v_initial[...])
    start = dot(time_high, first_high) + dot(time_high, first_low) + dot(time_low, first_high)
    inv_high, inv_low = halves(v_inverse[...])
    inv_node[:E, :] = dot(by_node[...], inv_high).astype(BF16)
    inv_node[E:, :] = dot(by_node[...], inv_low).astype(BF16)
    out_link = moved[0:8, :] * 256.0 + moved[8:16, :]
    for way in range(2):
        at = slice(way * PEER, way * PEER + PEER)
        far_send[way, 0:8, :] = out_link[:, at]
        far_send[way, 8:16, :] = moved[16:24, at]
        far_send[way, 16:24, :] = codes[24:32, at]
    count = jnp.where(slab > 0, 1, 0) + jnp.where(slab < n_slab - 1, 1, 0) + 4
    pl.semaphore_wait(barrier, count)
    for copy in far_copies:
        copy.start()
    loads[6].wait()
    rhs_high, rhs_low = halves(v_source[...] + jnp.where(slab == 0, start, 0.0))
    first = dot(inv_node[:E, :], rhs_high) + dot(inv_node[:E, :], rhs_low) + dot(inv_node[E:, :], rhs_high)
    const_node[...] = first
    leaving = exported(first)
    send_out(0, leaving, False)
    for copy in skip_copies:
        copy.start()
    keep(0, first, False)

    turn_out_rows = moved[16:24, :].astype(jnp.int32)
    loads[7].wait()
    lift_all[:, :384] = v_lift[...]
    lift_all[:, 384:448] = v_lift_time[...].T
    lift_high, lift_low = halves(lift_all[...])
    node_high, node_low = halves(
        dot(inv_node[:E, :], lift_high) + dot(inv_node[:E, :], lift_low) + dot(inv_node[E:, :], lift_high)
    )
    for face in range(6):
        at = slice(face * E, face * E + E)
        link_rows[:, at] = jnp.broadcast_to(v_links[face : face + 1, :], (16, E))
        turn_rows[face] = jnp.broadcast_to(v_orient[face : face + 1, :], (8, E))
        turn_out[face] = jnp.broadcast_to(turn_out_rows[face : face + 1, :], (8, E))
        wanted = jnp.broadcast_to(out_link[face : face + 1, :].astype(jnp.int32), (2 * PEER, E))
        pick_near[:, at] = jnp.where(wanted == iota((2 * PEER, E), 0) + LOCAL, 1.0, 0.0).astype(BF16)
    one, zero = jnp.ones((16, E), BF16), jnp.zeros((16, E), BF16)
    for face in range(6):
        at = slice(face * E, face * E + E)
        for tile in range(TABLE // E):
            link = link_rows[:, at]
            keys = jnp.where(link >> 8 == tile, link & 255, -1).astype(F32).astype(BF16)
            for step in range(E // 16):
                row = (iota((16, E), 0) + step * 16).astype(F32).astype(BF16)
                base = tile * E + step * 16
                pick[base : base + 16, at] = jnp.where(keys == row, one, zero)
    lhs_node[:E, :] = dot(node_high, spread[...]).astype(BF16)
    lhs_node[E:, :] = dot(node_low, spread[...]).astype(BF16)

    def local_part(turn, lhs, const):
        for pair in range(32):
            for half in range(2):
                at = slice(half * 128, half * 128 + 128)
                one, two = split_pair(fresh[half, pair * 8 : pair * 8 + 8, :])
                nodes[2 * pair, :, at] = one
                nodes[2 * pair + 1, :, at] = two
        for face, members in enumerate(FACES):
            for half in range(8):
                rows = [nodes[i * 16 + j * 4 + k] for i, j, k in members[2 * half : 2 * half + 2]]
                table[half * 16 : half * 16 + 16, face * E : face * E + E] = jnp.concatenate(
                    rows, axis=0
                ).astype(BF16)
        for face in range(6):
            at = slice(face * E, face * E + E)
            store_rows(nbr, face, oriented(dot(table[:, :LOCAL], pick[:LOCAL, at]), turn_rows[face]))
        sums = const[...] + apply(lhs, nbr, 0, NBR)

        @pl.when(slab > 0)
        def _():
            top_copy(turn).wait_recv()
            high, low = halves(top_arrived[turn])
            nbr[NBR : NBR + 64, :] = high
            nbr[NBR + 64 :, :] = low

        return sums + apply(lhs, nbr, NBR, K)

    def store_rows(ref, face, tiles):
        for half in range(8):
            row = face * 128 + half * 16
            ref[row : row + 16, :] = jnp.concatenate(tiles[2 * half : 2 * half + 2], axis=0).astype(BF16)

    def receive(turn):
        for copy in space_copies(turn):
            copy.wait_recv()
        for way in range(2):
            for half in range(8):
                rows = slice(half * 8, half * 8 + 8)
                pair = split_pair(arrived[turn, way, rows, :] + extra[way, rows, :])
                table[
                    half * 16 : half * 16 + 16, LOCAL + way * PEER : LOCAL + way * PEER + PEER
                ] = jnp.concatenate(pair, axis=0).astype(BF16)

    def remote_part(chosen, base, turns, columns=lambda: table[:, LOCAL:], depth=2 * PEER):
        for face in (0, 2, 4):
            block = dot(columns(), chosen[base : base + depth, face * E : face * E + 2 * E])
            store_rows(nbr_far, face, oriented(block[:, :E], turns[face]))
            store_rows(nbr_far, face + 1, oriented(block[:, E:], turns[face + 1]))


    def local_sums(turn):
        so_far = local_part(turn, lhs_node, const_node)
        own[...] = so_far
        own_out[...] = exported(so_far)

    def update(turn):
        @pl.when(space >= 0)
        def _():
            remote_part(pick, LOCAL, turn_rows)

        @pl.when(slab >= 0)
        def _():
            keep(turn + 1, own[...] + apply(lhs_node, nbr_far, 0, NBR))

    local_sums(0)
    send_out(1, own_out[...])
    for copy in far_copies:
        copy.wait_recv()
    side = jnp.where(iota((8, E), 1) < PEER, 0, 2 * PEER)
    for face in range(6):
        at = slice(face * E, face * E + E)
        link = jnp.concatenate([far_arrived[way, face : face + 1, :] for way in range(2)], axis=1).astype(jnp.int32)
        turned = jnp.concatenate([far_arrived[way, 8 + face : 9 + face, :] for way in range(2)], axis=1)
        far_turn[face] = jnp.broadcast_to(turned.astype(jnp.int32), (8, E))
        row = jnp.where(link >= LOCAL, link - LOCAL + side[0:1, :], -1)
        wanted = jnp.broadcast_to(row, (4 * PEER, E))
        far_pick[:, at] = jnp.where(wanted == iota((4 * PEER, E), 0), 1.0, 0.0).astype(BF16)
    receive(0)
    update(0)
    for copy in skip_copies:
        copy.wait_recv()
    for at, part in enumerate((skip_arrived.at[0], send.at[0, 0], send.at[0, 1], skip_arrived.at[1])):
        for half in range(8):
            pair = split_pair(part[half * 8 : half * 8 + 8, :])
            far_table[half * 16 : half * 16 + 16, at * PEER : at * PEER + PEER] = jnp.concatenate(
                pair, axis=0
            ).astype(BF16)
    remote_part(far_pick, 0, far_turn, lambda: far_table[...], 4 * PEER)
    face_code = jnp.concatenate([far_arrived[way, 16:17, :] for way in range(2)], axis=1).astype(jnp.int32)
    added = face_traces(apply(lhs_node, nbr_far, 0, NBR), jnp.broadcast_to(face_code, (8, E)))
    for half, rows in enumerate(added):
        extra[0, half * 8 : half * 8 + 8, :] = rows[:, :PEER]
        extra[1, half * 8 : half * 8 + 8, :] = rows[:, PEER:]

    @pl.loop(1, ROUNDS - 1)
    def _(turn):
        local_sums(turn)
        receive(turn)
        extra[...] = jnp.zeros((2, 64, PEER), F32)
        remote_part(pick_near, 0, turn_out)

        @pl.when(slab >= 0)
        def _():
            send_out(turn + 1, own_out[...] + apply(lhs_node, nbr_far, 0, NBR))

        update(turn)

    lhs_time[:E, :] = dot(by_time[...], lhs_node[:E, :]).astype(BF16)
    lhs_time[E:, :] = dot(by_time[...], lhs_node[E:, :]).astype(BF16)
    high, low = halves(const_node[...])
    const_time[...] = dot(by_time[...], high) + dot(by_time[...], low)
    own[...] = local_part(ROUNDS - 1, lhs_time, const_time)
    receive(ROUNDS - 1)
    remote_part(pick, LOCAL, turn_rows)

    @pl.when(slab >= 0)
    def _():
        out[0] = own[...] + apply(lhs_time, nbr_far, 0, NBR)

    for copy in space_copies(ROUNDS - 1) + far_copies + skip_copies:
        copy.wait_send()

    @pl.when(slab < n_slab - 1)
    def _():
        top_copy(ROUNDS - 1).wait_send()


def body(n_space, n_slab, source, initial, inverse, lift, lift_time, links, orient, exports, counts):
    hbm = pl.BlockSpec(memory_space=pltpu.HBM)
    arrays = (source, initial, inverse, lift, lift_time.T, links, orient, exports.reshape(1, E))
    arrays = [pltpu.with_memory_space_constraint(array, pltpu.HBM) for array in arrays]
    vmem = pltpu.VMEM
    dma = pltpu.SemaphoreType.DMA
    state = pl.pallas_call(
        functools.partial(kernel, n_space, n_slab),
        name="window",
        out_shape=jax.ShapeDtypeStruct((1, 256, E), F32),
        in_specs=[hbm] * 8,
        out_specs=pl.BlockSpec(memory_space=pltpu.VMEM),
        scratch_shapes=[
            vmem((256, E), F32),
            vmem((64, E), F32),
            vmem((256, 256), F32),
            vmem((256, 384), F32),
            vmem((64, 256), F32),
            vmem((6, E), jnp.int32),
            vmem((6, E), jnp.int32),
            vmem((1, E), jnp.int32),
            vmem((TABLE, LOCAL), BF16),
            vmem((2 * PEER, LOCAL), BF16),
            vmem((128, TABLE), BF16),
            vmem((K, E), BF16),
            vmem((NBR, E), BF16),
            vmem((512, K), BF16),
            vmem((512, K), BF16),
            vmem((512, 256), BF16),
            vmem((256, E), F32),
            vmem((256, E), F32),
            vmem((256, 256), BF16),
            vmem((256, 256), BF16),
            vmem((256, E), F32),
            vmem((256, E), F32),
            vmem((256, 512), F32),
            vmem((512, K), BF16),
            vmem((16, LOCAL), jnp.int32),
            vmem((6, 8, E), jnp.int32),
            vmem((6, 8, E), jnp.int32),
            vmem((32, E), F32),
            vmem((E, E), BF16),
            vmem((64, 8, E), F32),
            vmem((2, 256, 128), F32),
            vmem((ROUNDS, 2, 64, PEER), F32),
            vmem((ROUNDS, 2, 64, PEER), F32),
            vmem((ROUNDS, 64, E), F32),
            vmem((ROUNDS, 64, E), F32),
            vmem((2, 24, PEER), F32),
            vmem((2, 24, PEER), F32),
            vmem((2, 64, PEER), F32),
            vmem((4 * PEER, LOCAL), BF16),
            vmem((128, 4 * PEER), BF16),
            vmem((6, 8, E), jnp.int32),
            vmem((2, 64, PEER), F32),
            dma((8,)),
            dma((2,)),
            dma((ROUNDS, 2)),
            dma,
            dma((ROUNDS,)),
            dma((2, 2)),
            dma((2, 2)),
        ],
        compiler_params=pltpu.CompilerParams(
            collective_id=0, has_side_effects=True, vmem_limit_bytes=48 * 1024 * 1024
        ),
    )(*arrays)
    live = jnp.arange(E, dtype=jnp.int32) < counts[0]
    return jnp.where(live[None, None, :], state, 0.0)


def solution(mesh):
    return jax.shard_map(
        functools.partial(body, mesh.shape["space"], mesh.shape["slab"]),
        mesh=mesh,
        in_specs=(
            P("slab", None, "space"),
            P(None, "space"),
            P(),
            P(),
            P(),
            P(None, "space"),
            P(None, "space"),
            P("space"),
            P("space"),
        ),
        out_specs=P("slab", None, "space"),
        check_vma=False,
    )
```

```python
import functools

import jax
import jax.numpy as jnp
from jax import lax
from jax.experimental import pallas as pl
from jax.experimental.pallas import tpu as pltpu
from jax.sharding import PartitionSpec as P

ROUNDS = 5
E = 256
PEER = 128
LOCAL = 6 * E
TABLE = LOCAL + 2 * PEER
NBR = 6 * 128
K = NBR + 128
F32 = jnp.float32
BF16 = jnp.bfloat16
HIGHEST = lax.Precision.HIGHEST
MESH = pl.DeviceIdType.MESH

FACES = (
    [(0, a, b) for a in range(4) for b in range(4)],
    [(3, a, b) for a in range(4) for b in range(4)],
    [(a, 0, b) for a in range(4) for b in range(4)],
    [(a, 3, b) for a in range(4) for b in range(4)],
    [(a, b, 0) for a in range(4) for b in range(4)],
    [(a, b, 3) for a in range(4) for b in range(4)],
)


def iota(shape, dim):
    return lax.broadcasted_iota(jnp.int32, shape, dim)


def dot(a, b):
    return jnp.dot(a, b, preferred_element_type=F32)


def halves(x):
    high = x.astype(BF16)
    return high, (x - high.astype(F32)).astype(BF16)


def split_pair(x):
    low = iota(x.shape, 0) < 4
    turned = pltpu.roll(x, 4, 0)
    tiles = []
    for d in (jnp.where(low, x, turned), jnp.where(low, turned, x)):
        rest = d - d.astype(BF16).astype(F32)
        tiles.append(jnp.where(low, d, rest))
    return tiles


def apply(lhs, rows, begin, end):
    parts = []
    for at in (0, 128):
        parts.append(
            dot(lhs[at : at + 128, begin:end], rows[begin:end, :])
            + dot(lhs[E + at : E + at + 128, begin:end], rows[begin:end, :])
        )
    return jnp.concatenate(parts, axis=0)


def oriented(block, code):
    swap = (code & 4) > 0
    back_a = (code & 1) > 0
    back_b = (code & 2) > 0
    four = range(4)
    v = [[block[(a * 4 + b) * 8 : (a * 4 + b) * 8 + 8, :] for b in four] for a in four]
    v = [[v[a][b] if a == b else jnp.where(swap, v[b][a], v[a][b]) for b in four] for a in four]
    v = [[jnp.where(back_a, v[3 - a][b], v[a][b]) for b in four] for a in four]
    v = [[jnp.where(back_b, v[a][3 - b], v[a][b]) for b in four] for a in four]
    return [v[a][b] for a in four for b in four]


def face_traces(state, code):
    low = iota(code.shape, 0) < 4

    def tile(node):
        return state[node * 4 : node * 4 + 8, :]

    rows = []
    for half in range(8):
        a, b = half // 2, 2 * (half % 2)
        near, far = a * 16 + b * 4, a * 16 + b * 4 + 4
        choices = [
            tile(a * 4 + b),
            tile(48 + a * 4 + b),
            tile(a * 16 + b),
            tile(a * 16 + 12 + b),
            jnp.where(low, tile(near), pltpu.roll(tile(far), 4, 0)),
            jnp.where(low, pltpu.roll(tile(near + 2), 4, 0), tile(far + 2)),
        ]
        value = choices[0]
        for face in range(1, 6):
            value = jnp.where(code == face, choices[face], value)
        rows.append(value)
    return rows


def kernel(
    n_space,
    n_slab,
    source,
    initial,
    inverse,
    lift,
    lift_time,
    links,
    orient,
    exports,
    out,
    v_source,
    v_initial,
    v_inverse,
    v_lift,
    v_lift_time,
    v_links,
    v_orient,
    v_exports,
    pick,
    pick_near,
    table,
    nbr,
    nbr_far,
    lhs_node,
    lhs_time,
    inv_node,
    const_node,
    const_time,
    by_node,
    by_time,
    own,
    own_out,
    lift_all,
    spread,
    link_rows,
    turn_rows,
    turn_out,
    codes,
    select,
    nodes,
    fresh,
    send,
    arrived,
    top_send,
    top_arrived,
    far_send,
    far_arrived,
    skip_arrived,
    far_pick,
    far_table,
    far_turn,
    extra,
    in_sem,
    send_sem,
    recv_sem,
    top_send_sem,
    top_recv_sem,
    far_sem,
    skip_sem,
):
    space = lax.axis_index("space")
    slab = lax.axis_index("slab")
    upper = {"space": lax.rem(space + 1, n_space)}
    lower = {"space": lax.rem(space + n_space - 1, n_space)}
    second_upper = {"space": lax.rem(space + 2, n_space)}
    second_lower = {"space": lax.rem(space + n_space - 2, n_space)}

    loads = []
    for at, (src, dst) in enumerate(
        (
            (exports, v_exports),
            (links, v_links),
            (orient, v_orient),
            (lift_time, v_lift_time),
            (initial, v_initial),
            (inverse, v_inverse),
            (source.at[0], v_source),
            (lift, v_lift),
        )
    ):
        copy = pltpu.make_async_copy(src, dst, in_sem.at[at])
        copy.start()
        loads.append(copy)

    barrier = pltpu.get_barrier_semaphore()
    for peer in (lower, upper, second_lower, second_upper):
        pl.semaphore_signal(barrier, inc=1, device_id=peer, device_id_type=MESH)

    @pl.when(slab > 0)
    def _():
        pl.semaphore_signal(barrier, inc=1, device_id={"slab": slab - 1}, device_id_type=MESH)

    @pl.when(slab < n_slab - 1)
    def _():
        pl.semaphore_signal(barrier, inc=1, device_id={"slab": slab + 1}, device_id_type=MESH)

    def space_copies(turn):
        return [
            pltpu.make_async_remote_copy(
                src_ref=send.at[turn, way],
                dst_ref=arrived.at[turn, 1 - way],
                send_sem=send_sem.at[way],
                recv_sem=recv_sem.at[turn, 1 - way],
                device_id=peer,
                device_id_type=MESH,
            )
            for way, peer in ((0, lower), (1, upper))
        ]

    def other_copies(source_of, target, sems, peers):
        return [
            pltpu.make_async_remote_copy(
                src_ref=source_of(way),
                dst_ref=target.at[1 - way],
                send_sem=sems.at[0, way],
                recv_sem=sems.at[1, 1 - way],
                device_id=peer,
                device_id_type=MESH,
            )
            for way, peer in enumerate(peers)
        ]

    far_copies = other_copies(lambda way: far_send.at[way], far_arrived, far_sem, (lower, upper))
    skip_copies = other_copies(lambda way: send.at[0, way], skip_arrived, skip_sem, (second_lower, second_upper))

    def top_copy(turn):
        return pltpu.make_async_remote_copy(
            src_ref=top_send.at[turn],
            dst_ref=top_arrived.at[turn],
            send_sem=top_send_sem,
            recv_sem=top_recv_sem.at[turn],
            device_id={"slab": lax.rem(slab + 1, n_slab)},
            device_id_type=MESH,
        )

    def send_out(turn, state, turn_is_later=True):
        code = jnp.broadcast_to(v_exports[...] >> 8, (8, E))
        for half, rows in enumerate(face_traces(state, code)):
            send[turn, 0, half * 8 : half * 8 + 8, :] = rows[:, :PEER]
            send[turn, 1, half * 8 : half * 8 + 8, :] = rows[:, PEER:]
        if not turn_is_later:
            return
        for copy in space_copies(turn - 1):
            copy.wait_send()
        for copy in space_copies(turn):
            copy.start()

    def keep(turn, state, turn_is_later=True):
        for half in range(2):
            fresh[half] = state[:, half * 128 : half * 128 + 128]
        for half in range(2):
            top_send[turn, :, half * 128 : half * 128 + 128] = fresh[half, pl.ds(3, 64, stride=4), :]
        if not turn_is_later:
            return

        @pl.when(slab < n_slab - 1)
        def _():
            top_copy(turn - 1).wait_send()
            top_copy(turn).start()

    def exported(state):
        high, low = halves(state)
        return dot(high, select[...]) + dot(low, select[...])

    row, column = iota((E, E), 0), iota((E, E), 1)
    by_node[...] = jnp.where(column == (row & 3) * 64 + (row >> 2), 1.0, 0.0).astype(BF16)
    by_time[...] = jnp.where(column == (row & 63) * 4 + (row >> 6), 1.0, 0.0).astype(BF16)
    column = iota((512, K), 1)
    face_source = ((column & 3) * 16 + ((column >> 3) & 15)) * 6 + (column >> 7)
    wanted_row = jnp.where(column < NBR, face_source, 384 + (column & 63))
    spread[...] = jnp.where(iota((512, K), 0) == wanted_row, 1.0, 0.0).astype(BF16)
    codes[...] = jnp.zeros((32, E), F32)
    nbr[NBR:, :] = jnp.zeros((128, E), BF16)
    nbr_far[NBR:, :] = jnp.zeros((128, E), BF16)
    lift_all[:, 384:] = jnp.zeros((E, 128), F32)

    for load in loads[:6]:
        load.wait()
    element = jnp.broadcast_to(v_exports[...] & 255, (E, E))
    select[...] = jnp.where(element == iota((E, E), 0), 1.0, 0.0).astype(BF16)
    codes[0:6, :] = (v_links[...] >> 8).astype(F32)
    codes[8:14, :] = (v_links[...] & 255).astype(F32)
    codes[16:22, :] = v_orient[...].astype(F32)
    codes[24:25, :] = (v_exports[...] >> 8).astype(F32)
    moved = dot(codes[0:24, :].astype(BF16), select[...])
    time_high, time_low = halves(v_lift_time[...].T)
    first_high, first_low = halves(v_initial[...])
    start = dot(time_high, first_high) + dot(time_high, first_low) + dot(time_low, first_high)
    inv_high, inv_low = halves(v_inverse[...])
    inv_node[:E, :] = dot(by_node[...], inv_high).astype(BF16)
    inv_node[E:, :] = dot(by_node[...], inv_low).astype(BF16)
    out_link = moved[0:8, :] * 256.0 + moved[8:16, :]
    for way in range(2):
        at = slice(way * PEER, way * PEER + PEER)
        far_send[way, 0:8, :] = out_link[:, at]
        far_send[way, 8:16, :] = moved[16:24, at]
        far_send[way, 16:24, :] = codes[24:32, at]
    loads[6].wait()
    rhs_high, rhs_low = halves(v_source[...] + jnp.where(slab == 0, start, 0.0))
    first = dot(inv_node[:E, :], rhs_high) + dot(inv_node[:E, :], rhs_low) + dot(inv_node[E:, :], rhs_high)
    const_node[...] = first
    leaving = exported(first)
    keep(0, first, False)
    send_out(0, leaving, False)
    count = jnp.where(slab > 0, 1, 0) + jnp.where(slab < n_slab - 1, 1, 0) + 4
    pl.semaphore_wait(barrier, count)
    for copy in space_copies(0):
        copy.start()

    @pl.when(slab < n_slab - 1)
    def _():
        top_copy(0).start()

    for copy in far_copies + skip_copies:
        copy.start()

    turn_out_rows = moved[16:24, :].astype(jnp.int32)
    loads[7].wait()
    lift_all[:, :384] = v_lift[...]
    lift_all[:, 384:448] = v_lift_time[...].T
    lift_high, lift_low = halves(lift_all[...])
    node_high, node_low = halves(
        dot(inv_node[:E, :], lift_high) + dot(inv_node[:E, :], lift_low) + dot(inv_node[E:, :], lift_high)
    )
    for face in range(6):
        at = slice(face * E, face * E + E)
        link_rows[:, at] = jnp.broadcast_to(v_links[face : face + 1, :], (16, E))
        turn_rows[face] = jnp.broadcast_to(v_orient[face : face + 1, :], (8, E))
        turn_out[face] = jnp.broadcast_to(turn_out_rows[face : face + 1, :], (8, E))
        wanted = jnp.broadcast_to(out_link[face : face + 1, :].astype(jnp.int32), (2 * PEER, E))
        pick_near[:, at] = jnp.where(wanted == iota((2 * PEER, E), 0) + LOCAL, 1.0, 0.0).astype(BF16)
    one, zero = jnp.ones((16, E), BF16), jnp.zeros((16, E), BF16)
    for face in range(6):
        at = slice(face * E, face * E + E)
        for tile in range(TABLE // E):
            link = link_rows[:, at]
            keys = jnp.where(link >> 8 == tile, link & 255, -1).astype(F32).astype(BF16)
            for step in range(E // 16):
                row = (iota((16, E), 0) + step * 16).astype(F32).astype(BF16)
                base = tile * E + step * 16
                pick[base : base + 16, at] = jnp.where(keys == row, one, zero)
    lhs_node[:E, :] = dot(node_high, spread[...]).astype(BF16)
    lhs_node[E:, :] = dot(node_low, spread[...]).astype(BF16)

    def local_part(turn, lhs, const):
        for pair in range(32):
            for half in range(2):
                at = slice(half * 128, half * 128 + 128)
                one, two = split_pair(fresh[half, pair * 8 : pair * 8 + 8, :])
                nodes[2 * pair, :, at] = one
                nodes[2 * pair + 1, :, at] = two
        for face, members in enumerate(FACES):
            for half in range(8):
                rows = [nodes[i * 16 + j * 4 + k] for i, j, k in members[2 * half : 2 * half + 2]]
                table[half * 16 : half * 16 + 16, face * E : face * E + E] = jnp.concatenate(
                    rows, axis=0
                ).astype(BF16)
        for face in range(6):
            at = slice(face * E, face * E + E)
            store_rows(nbr, face, oriented(dot(table[:, :LOCAL], pick[:LOCAL, at]), turn_rows[face]))
        return const[...] + apply(lhs, nbr, 0, NBR)

    def take_top(turn, for_exports=False):
        @pl.when(slab > 0)
        def _():
            top_copy(turn).wait_recv()
            high, low = halves(top_arrived[turn])
            nbr[NBR : NBR + 64, :] = high
            nbr[NBR + 64 :, :] = low
            if for_exports:
                nbr_far[NBR:, :] = dot(nbr[NBR:, :], select[...]).astype(BF16)

    def store_rows(ref, face, tiles):
        for half in range(8):
            row = face * 128 + half * 16
            ref[row : row + 16, :] = jnp.concatenate(tiles[2 * half : 2 * half + 2], axis=0).astype(BF16)

    def receive(turn, completed=False):
        for copy in space_copies(turn):
            copy.wait_recv()
        for way in range(2):
            for half in range(8):
                rows = slice(half * 8, half * 8 + 8)
                value = arrived[turn, way, rows, :]
                pair = split_pair(value + extra[way, rows, :] if completed else value)
                table[
                    half * 16 : half * 16 + 16, LOCAL + way * PEER : LOCAL + way * PEER + PEER
                ] = jnp.concatenate(pair, axis=0).astype(BF16)

    def remote_part(chosen, base, turns, columns=lambda: table[:, LOCAL:], depth=2 * PEER):
        for face in (0, 2, 4):
            block = dot(columns(), chosen[base : base + depth, face * E : face * E + 2 * E])
            store_rows(nbr_far, face, oriented(block[:, :E], turns[face]))
            store_rows(nbr_far, face + 1, oriented(block[:, E:], turns[face + 1]))


    def local_sums(turn, top_later=False):
        so_far = local_part(turn, lhs_node, const_node)
        if not top_later:
            take_top(turn)
            so_far += apply(lhs_node, nbr, NBR, K)
        own[...] = so_far
        own_out[...] = exported(so_far)

    def update(turn, depth=NBR):
        @pl.when(space >= 0)
        def _():
            remote_part(pick, LOCAL, turn_rows)
            if depth > NBR:
                nbr_far[NBR:, :] = nbr[NBR:, :]

        @pl.when(slab >= 0)
        def _():
            keep(turn + 1, own[...] + apply(lhs_node, nbr_far, 0, depth))

    local_sums(0)
    send_out(1, own_out[...])
    for copy in far_copies:
        copy.wait_recv()
    side = jnp.where(iota((8, E), 1) < PEER, 0, 2 * PEER)
    for face in range(6):
        at = slice(face * E, face * E + E)
        link = jnp.concatenate([far_arrived[way, face : face + 1, :] for way in range(2)], axis=1).astype(jnp.int32)
        turned = jnp.concatenate([far_arrived[way, 8 + face : 9 + face, :] for way in range(2)], axis=1)
        far_turn[face] = jnp.broadcast_to(turned.astype(jnp.int32), (8, E))
        row = jnp.where(link >= LOCAL, link - LOCAL + side[0:1, :], -1)
        wanted = jnp.broadcast_to(row, (4 * PEER, E))
        far_pick[:, at] = jnp.where(wanted == iota((4 * PEER, E), 0), 1.0, 0.0).astype(BF16)
    receive(0)
    update(0)
    for copy in skip_copies:
        copy.wait_recv()
    for at, part in enumerate((skip_arrived.at[0], send.at[0, 0], send.at[0, 1], skip_arrived.at[1])):
        for half in range(8):
            pair = split_pair(part[half * 8 : half * 8 + 8, :])
            far_table[half * 16 : half * 16 + 16, at * PEER : at * PEER + PEER] = jnp.concatenate(
                pair, axis=0
            ).astype(BF16)
    remote_part(far_pick, 0, far_turn, lambda: far_table[...], 4 * PEER)
    face_code = jnp.concatenate([far_arrived[way, 16:17, :] for way in range(2)], axis=1).astype(jnp.int32)
    added = face_traces(apply(lhs_node, nbr_far, 0, NBR), jnp.broadcast_to(face_code, (8, E)))
    for half, rows in enumerate(added):
        extra[0, half * 8 : half * 8 + 8, :] = rows[:, :PEER]
        extra[1, half * 8 : half * 8 + 8, :] = rows[:, PEER:]

    def advance(turn, top_later=False):
        depth = K if top_later else NBR
        local_sums(turn, top_later)
        receive(turn, top_later)
        remote_part(pick_near, 0, turn_out)
        if top_later:
            take_top(turn, True)

        @pl.when(slab >= 0)
        def _():
            send_out(turn + 1, own_out[...] + apply(lhs_node, nbr_far, 0, depth))

        update(turn, depth)

    advance(1, True)

    @pl.loop(2, ROUNDS - 1)
    def _(turn):
        advance(turn)

    lhs_time[:E, :] = dot(by_time[...], lhs_node[:E, :]).astype(BF16)
    lhs_time[E:, :] = dot(by_time[...], lhs_node[E:, :]).astype(BF16)
    high, low = halves(const_node[...])
    const_time[...] = dot(by_time[...], high) + dot(by_time[...], low)
    own[...] = local_part(ROUNDS - 1, lhs_time, const_time)
    take_top(ROUNDS - 1)
    own[...] += apply(lhs_time, nbr, NBR, K)
    receive(ROUNDS - 1)
    remote_part(pick, LOCAL, turn_rows)

    @pl.when(slab >= 0)
    def _():
        out[0] = own[...] + apply(lhs_time, nbr_far, 0, NBR)

    for copy in space_copies(ROUNDS - 1) + far_copies + skip_copies:
        copy.wait_send()

    @pl.when(slab < n_slab - 1)
    def _():
        top_copy(ROUNDS - 1).wait_send()


def body(n_space, n_slab, source, initial, inverse, lift, lift_time, links, orient, exports, counts):
    hbm = pl.BlockSpec(memory_space=pltpu.HBM)
    arrays = (source, initial, inverse, lift, lift_time.T, links, orient, exports.reshape(1, E))
    arrays = [pltpu.with_memory_space_constraint(array, pltpu.HBM) for array in arrays]
    vmem = pltpu.VMEM
    dma = pltpu.SemaphoreType.DMA
    state = pl.pallas_call(
        functools.partial(kernel, n_space, n_slab),
        name="window",
        out_shape=jax.ShapeDtypeStruct((1, 256, E), F32),
        in_specs=[hbm] * 8,
        out_specs=pl.BlockSpec(memory_space=pltpu.VMEM),
        scratch_shapes=[
            vmem((256, E), F32),
            vmem((64, E), F32),
            vmem((256, 256), F32),
            vmem((256, 384), F32),
            vmem((64, 256), F32),
            vmem((6, E), jnp.int32),
            vmem((6, E), jnp.int32),
            vmem((1, E), jnp.int32),
            vmem((TABLE, LOCAL), BF16),
            vmem((2 * PEER, LOCAL), BF16),
            vmem((128, TABLE), BF16),
            vmem((K, E), BF16),
            vmem((K, E), BF16),
            vmem((512, K), BF16),
            vmem((512, K), BF16),
            vmem((512, 256), BF16),
            vmem((256, E), F32),
            vmem((256, E), F32),
            vmem((256, 256), BF16),
            vmem((256, 256), BF16),
            vmem((256, E), F32),
            vmem((256, E), F32),
            vmem((256, 512), F32),
            vmem((512, K), BF16),
            vmem((16, LOCAL), jnp.int32),
            vmem((6, 8, E), jnp.int32),
            vmem((6, 8, E), jnp.int32),
            vmem((32, E), F32),
            vmem((E, E), BF16),
            vmem((64, 8, E), F32),
            vmem((2, 256, 128), F32),
            vmem((ROUNDS, 2, 64, PEER), F32),
            vmem((ROUNDS, 2, 64, PEER), F32),
            vmem((ROUNDS, 64, E), F32),
            vmem((ROUNDS, 64, E), F32),
            vmem((2, 24, PEER), F32),
            vmem((2, 24, PEER), F32),
            vmem((2, 64, PEER), F32),
            vmem((4 * PEER, LOCAL), BF16),
            vmem((128, 4 * PEER), BF16),
            vmem((6, 8, E), jnp.int32),
            vmem((2, 64, PEER), F32),
            dma((8,)),
            dma((2,)),
            dma((ROUNDS, 2)),
            dma,
            dma((ROUNDS,)),
            dma((2, 2)),
            dma((2, 2)),
        ],
        compiler_params=pltpu.CompilerParams(
            collective_id=0, has_side_effects=True, vmem_limit_bytes=48 * 1024 * 1024
        ),
    )(*arrays)
    live = jnp.arange(E, dtype=jnp.int32) < counts[0]
    return jnp.where(live[None, None, :], state, 0.0)


def solution(mesh):
    return jax.shard_map(
        functools.partial(body, mesh.shape["space"], mesh.shape["slab"]),
        mesh=mesh,
        in_specs=(
            P("slab", None, "space"),
            P(None, "space"),
            P(),
            P(),
            P(),
            P(None, "space"),
            P(None, "space"),
            P("space"),
            P("space"),
        ),
        out_specs=P("slab", None, "space"),
        check_vma=False,
    )
```

```python
import functools

import jax
import jax.numpy as jnp
from jax import lax
from jax.experimental import pallas as pl
from jax.experimental.pallas import tpu as pltpu
from jax.sharding import PartitionSpec as P

ROUNDS = 5
E = 256
PEER = 128
LOCAL = 6 * E
TABLE = LOCAL + 2 * PEER
NBR = 6 * 128
K = NBR + 128
F32 = jnp.float32
BF16 = jnp.bfloat16
HIGHEST = lax.Precision.HIGHEST
MESH = pl.DeviceIdType.MESH

FACES = (
    [(0, a, b) for a in range(4) for b in range(4)],
    [(3, a, b) for a in range(4) for b in range(4)],
    [(a, 0, b) for a in range(4) for b in range(4)],
    [(a, 3, b) for a in range(4) for b in range(4)],
    [(a, b, 0) for a in range(4) for b in range(4)],
    [(a, b, 3) for a in range(4) for b in range(4)],
)


def iota(shape, dim):
    return lax.broadcasted_iota(jnp.int32, shape, dim)


def dot(a, b):
    return jnp.dot(a, b, preferred_element_type=F32)


def halves(x):
    high = x.astype(BF16)
    return high, (x - high.astype(F32)).astype(BF16)


def split_pair(x):
    low = iota(x.shape, 0) < 4
    turned = pltpu.roll(x, 4, 0)
    tiles = []
    for d in (jnp.where(low, x, turned), jnp.where(low, turned, x)):
        rest = d - d.astype(BF16).astype(F32)
        tiles.append(jnp.where(low, d, rest))
    return tiles


def apply(lhs, rows, begin, end):
    parts = []
    for at in (0, 128):
        parts.append(
            dot(lhs[at : at + 128, begin:end], rows[begin:end, :])
            + dot(lhs[E + at : E + at + 128, begin:end], rows[begin:end, :])
        )
    return jnp.concatenate(parts, axis=0)


def oriented(block, code):
    swap = (code & 4) > 0
    back_a = (code & 1) > 0
    back_b = (code & 2) > 0
    four = range(4)
    v = [[block[(a * 4 + b) * 8 : (a * 4 + b) * 8 + 8, :] for b in four] for a in four]
    v = [[v[a][b] if a == b else jnp.where(swap, v[b][a], v[a][b]) for b in four] for a in four]
    v = [[jnp.where(back_a, v[3 - a][b], v[a][b]) for b in four] for a in four]
    v = [[jnp.where(back_b, v[a][3 - b], v[a][b]) for b in four] for a in four]
    return [v[a][b] for a in four for b in four]


def face_traces(state, code):
    low = iota(code.shape, 0) < 4

    def tile(node):
        return state[node * 4 : node * 4 + 8, :]

    rows = []
    for half in range(8):
        a, b = half // 2, 2 * (half % 2)
        near, far = a * 16 + b * 4, a * 16 + b * 4 + 4
        choices = [
            tile(a * 4 + b),
            tile(48 + a * 4 + b),
            tile(a * 16 + b),
            tile(a * 16 + 12 + b),
            jnp.where(low, tile(near), pltpu.roll(tile(far), 4, 0)),
            jnp.where(low, pltpu.roll(tile(near + 2), 4, 0), tile(far + 2)),
        ]
        value = choices[0]
        for face in range(1, 6):
            value = jnp.where(code == face, choices[face], value)
        rows.append(value)
    return rows


def kernel(
    n_space,
    n_slab,
    source,
    initial,
    inverse,
    lift,
    lift_time,
    links,
    orient,
    exports,
    out,
    v_source,
    v_initial,
    v_inverse,
    v_lift,
    v_lift_time,
    v_links,
    v_orient,
    v_exports,
    pick,
    pick_near,
    table,
    nbr,
    nbr_far,
    lhs_node,
    lhs_time,
    inv_node,
    const_node,
    const_time,
    by_node,
    by_time,
    own,
    own_out,
    lift_all,
    spread,
    link_rows,
    turn_rows,
    turn_out,
    codes,
    select,
    nodes,
    fresh,
    send,
    arrived,
    top_send,
    top_arrived,
    far_send,
    far_arrived,
    skip_arrived,
    far_pick,
    far_table,
    far_turn,
    extra,
    in_sem,
    send_sem,
    recv_sem,
    top_send_sem,
    top_recv_sem,
    far_sem,
    skip_sem,
):
    space = lax.axis_index("space")
    slab = lax.axis_index("slab")
    upper = {"space": lax.rem(space + 1, n_space)}
    lower = {"space": lax.rem(space + n_space - 1, n_space)}

    loads = []
    for at, (src, dst) in enumerate(
        (
            (exports, v_exports),
            (links, v_links),
            (orient, v_orient),
            (lift_time, v_lift_time),
            (initial, v_initial),
            (inverse, v_inverse),
            (source.at[0], v_source),
            (lift, v_lift),
        )
    ):
        copy = pltpu.make_async_copy(src, dst, in_sem.at[at])
        copy.start()
        loads.append(copy)

    barrier = pltpu.get_barrier_semaphore()
    for peer in (lower, upper):
        pl.semaphore_signal(barrier, inc=1, device_id=peer, device_id_type=MESH)

    @pl.when(slab > 0)
    def _():
        pl.semaphore_signal(barrier, inc=1, device_id={"slab": slab - 1}, device_id_type=MESH)

    @pl.when(slab < n_slab - 1)
    def _():
        pl.semaphore_signal(barrier, inc=1, device_id={"slab": slab + 1}, device_id_type=MESH)

    def space_copies(turn):
        return [
            pltpu.make_async_remote_copy(
                src_ref=send.at[turn, way],
                dst_ref=arrived.at[turn, 1 - way],
                send_sem=send_sem.at[way],
                recv_sem=recv_sem.at[turn, 1 - way],
                device_id=peer,
                device_id_type=MESH,
            )
            for way, peer in ((0, lower), (1, upper))
        ]

    def other_copies(source_of, target, sems, peers):
        return [
            pltpu.make_async_remote_copy(
                src_ref=source_of(way),
                dst_ref=target.at[1 - way],
                send_sem=sems.at[0, way],
                recv_sem=sems.at[1, 1 - way],
                device_id=peer,
                device_id_type=MESH,
            )
            for way, peer in enumerate(peers)
        ]

    far_copies = other_copies(lambda way: far_send.at[way], far_arrived, far_sem, (lower, upper))

    def first_arrival(side):
        return pltpu.make_async_remote_copy(
            src_ref=send.at[0, 1 - side],
            dst_ref=arrived.at[0, side],
            send_sem=send_sem.at[1 - side],
            recv_sem=recv_sem.at[0, side],
            device_id=lower,
            device_id_type=MESH,
        )

    def relay(side):
        return pltpu.make_async_remote_copy(
            src_ref=arrived.at[0, side],
            dst_ref=skip_arrived.at[side],
            send_sem=skip_sem.at[0, side],
            recv_sem=skip_sem.at[1, side],
            device_id={"space": lax.rem(space + n_space + 1 - 2 * side, n_space)},
            device_id_type=MESH,
        )

    near_side = lax.rem(space + 1, 2)

    def top_copy(turn):
        return pltpu.make_async_remote_copy(
            src_ref=top_send.at[turn],
            dst_ref=top_arrived.at[turn],
            send_sem=top_send_sem,
            recv_sem=top_recv_sem.at[turn],
            device_id={"slab": lax.rem(slab + 1, n_slab)},
            device_id_type=MESH,
        )

    def send_out(turn, state, turn_is_later=True):
        code = jnp.broadcast_to(v_exports[...] >> 8, (8, E))
        for half, rows in enumerate(face_traces(state, code)):
            send[turn, 0, half * 8 : half * 8 + 8, :] = rows[:, :PEER]
            send[turn, 1, half * 8 : half * 8 + 8, :] = rows[:, PEER:]
        if not turn_is_later:
            return
        for copy in space_copies(turn - 1):
            copy.wait_send()
        for copy in space_copies(turn):
            copy.start()

    def keep(turn, state, turn_is_later=True):
        for half in range(2):
            fresh[half] = state[:, half * 128 : half * 128 + 128]
        for half in range(2):
            top_send[turn, :, half * 128 : half * 128 + 128] = fresh[half, pl.ds(3, 64, stride=4), :]
        if not turn_is_later:
            return

        @pl.when(slab < n_slab - 1)
        def _():
            top_copy(turn - 1).wait_send()
            top_copy(turn).start()

    def exported(state):
        high, low = halves(state)
        return dot(high, select[...]) + dot(low, select[...])

    row, column = iota((E, E), 0), iota((E, E), 1)
    by_node[...] = jnp.where(column == (row & 3) * 64 + (row >> 2), 1.0, 0.0).astype(BF16)
    by_time[...] = jnp.where(column == (row & 63) * 4 + (row >> 6), 1.0, 0.0).astype(BF16)
    column = iota((512, K), 1)
    face_source = ((column & 3) * 16 + ((column >> 3) & 15)) * 6 + (column >> 7)
    wanted_row = jnp.where(column < NBR, face_source, 384 + (column & 63))
    spread[...] = jnp.where(iota((512, K), 0) == wanted_row, 1.0, 0.0).astype(BF16)
    codes[...] = jnp.zeros((32, E), F32)
    nbr[NBR:, :] = jnp.zeros((128, E), BF16)
    nbr_far[NBR:, :] = jnp.zeros((128, E), BF16)
    lift_all[:, 384:] = jnp.zeros((E, 128), F32)

    for load in loads[:6]:
        load.wait()
    element = jnp.broadcast_to(v_exports[...] & 255, (E, E))
    select[...] = jnp.where(element == iota((E, E), 0), 1.0, 0.0).astype(BF16)
    codes[0:6, :] = (v_links[...] >> 8).astype(F32)
    codes[8:14, :] = (v_links[...] & 255).astype(F32)
    codes[16:22, :] = v_orient[...].astype(F32)
    codes[24:25, :] = (v_exports[...] >> 8).astype(F32)
    moved = dot(codes[0:24, :].astype(BF16), select[...])
    time_high, time_low = halves(v_lift_time[...].T)
    first_high, first_low = halves(v_initial[...])
    start = dot(time_high, first_high) + dot(time_high, first_low) + dot(time_low, first_high)
    inv_high, inv_low = halves(v_inverse[...])
    inv_node[:E, :] = dot(by_node[...], inv_high).astype(BF16)
    inv_node[E:, :] = dot(by_node[...], inv_low).astype(BF16)
    out_link = moved[0:8, :] * 256.0 + moved[8:16, :]
    for way in range(2):
        at = slice(way * PEER, way * PEER + PEER)
        far_send[way, 0:8, :] = out_link[:, at]
        far_send[way, 8:16, :] = moved[16:24, at]
        far_send[way, 16:24, :] = codes[24:32, at]
    loads[6].wait()
    rhs_high, rhs_low = halves(v_source[...] + jnp.where(slab == 0, start, 0.0))
    first = dot(inv_node[:E, :], rhs_high) + dot(inv_node[:E, :], rhs_low) + dot(inv_node[E:, :], rhs_high)
    const_node[...] = first
    leaving = exported(first)
    keep(0, first, False)
    send_out(0, leaving, False)
    count = jnp.where(slab > 0, 1, 0) + jnp.where(slab < n_slab - 1, 1, 0) + 2
    pl.semaphore_wait(barrier, count)
    for copy in space_copies(0):
        copy.start()

    @pl.when(slab < n_slab - 1)
    def _():
        top_copy(0).start()

    for copy in far_copies:
        copy.start()

    turn_out_rows = moved[16:24, :].astype(jnp.int32)
    loads[7].wait()
    lift_all[:, :384] = v_lift[...]
    lift_all[:, 384:448] = v_lift_time[...].T
    lift_high, lift_low = halves(lift_all[...])
    node_high, node_low = halves(
        dot(inv_node[:E, :], lift_high) + dot(inv_node[:E, :], lift_low) + dot(inv_node[E:, :], lift_high)
    )
    for face in range(6):
        at = slice(face * E, face * E + E)
        link_rows[:, at] = jnp.broadcast_to(v_links[face : face + 1, :], (16, E))
        turn_rows[face] = jnp.broadcast_to(v_orient[face : face + 1, :], (8, E))
        turn_out[face] = jnp.broadcast_to(turn_out_rows[face : face + 1, :], (8, E))
        wanted = jnp.broadcast_to(out_link[face : face + 1, :].astype(jnp.int32), (2 * PEER, E))
        pick_near[:, at] = jnp.where(wanted == iota((2 * PEER, E), 0) + LOCAL, 1.0, 0.0).astype(BF16)
    one, zero = jnp.ones((16, E), BF16), jnp.zeros((16, E), BF16)
    for face in range(6):
        at = slice(face * E, face * E + E)
        for tile in range(TABLE // E):
            link = link_rows[:, at]
            keys = jnp.where(link >> 8 == tile, link & 255, -1).astype(F32).astype(BF16)
            for step in range(E // 16):
                row = (iota((16, E), 0) + step * 16).astype(F32).astype(BF16)
                base = tile * E + step * 16
                pick[base : base + 16, at] = jnp.where(keys == row, one, zero)
    lhs_node[:E, :] = dot(node_high, spread[...]).astype(BF16)
    lhs_node[E:, :] = dot(node_low, spread[...]).astype(BF16)
    first_arrival(near_side).wait_recv()
    relay(near_side).start()

    def local_part(turn, lhs, const):
        for pair in range(32):
            for half in range(2):
                at = slice(half * 128, half * 128 + 128)
                one, two = split_pair(fresh[half, pair * 8 : pair * 8 + 8, :])
                nodes[2 * pair, :, at] = one
                nodes[2 * pair + 1, :, at] = two
        for face, members in enumerate(FACES):
            for half in range(8):
                rows = [nodes[i * 16 + j * 4 + k] for i, j, k in members[2 * half : 2 * half + 2]]
                table[half * 16 : half * 16 + 16, face * E : face * E + E] = jnp.concatenate(
                    rows, axis=0
                ).astype(BF16)
        for face in range(6):
            at = slice(face * E, face * E + E)
            store_rows(nbr, face, oriented(dot(table[:, :LOCAL], pick[:LOCAL, at]), turn_rows[face]))
        return const[...] + apply(lhs, nbr, 0, NBR)

    def take_top(turn, for_exports=False):
        @pl.when(slab > 0)
        def _():
            top_copy(turn).wait_recv()
            high, low = halves(top_arrived[turn])
            nbr[NBR : NBR + 64, :] = high
            nbr[NBR + 64 :, :] = low
            if for_exports:
                nbr_far[NBR:, :] = dot(nbr[NBR:, :], select[...]).astype(BF16)

    def store_rows(ref, face, tiles):
        for half in range(8):
            row = face * 128 + half * 16
            ref[row : row + 16, :] = jnp.concatenate(tiles[2 * half : 2 * half + 2], axis=0).astype(BF16)

    def receive(turn, completed=False):
        if completed is None:
            first_arrival(1 - near_side).wait_recv()
            relay(1 - near_side).start()
        else:
            for copy in space_copies(turn):
                copy.wait_recv()
        for way in range(2):
            for half in range(8):
                rows = slice(half * 8, half * 8 + 8)
                value = arrived[turn, way, rows, :]
                pair = split_pair(value + extra[way, rows, :] if completed else value)
                table[
                    half * 16 : half * 16 + 16, LOCAL + way * PEER : LOCAL + way * PEER + PEER
                ] = jnp.concatenate(pair, axis=0).astype(BF16)

    def remote_part(chosen, base, turns, columns=lambda: table[:, LOCAL:], depth=2 * PEER):
        for face in (0, 2, 4):
            block = dot(columns(), chosen[base : base + depth, face * E : face * E + 2 * E])
            store_rows(nbr_far, face, oriented(block[:, :E], turns[face]))
            store_rows(nbr_far, face + 1, oriented(block[:, E:], turns[face + 1]))


    def local_sums(turn, top_later=False):
        so_far = local_part(turn, lhs_node, const_node)
        if not top_later:
            take_top(turn)
            so_far += apply(lhs_node, nbr, NBR, K)
        own[...] = so_far
        own_out[...] = exported(so_far)

    def update(turn, depth=NBR):
        @pl.when(space >= 0)
        def _():
            remote_part(pick, LOCAL, turn_rows)
            if depth > NBR:
                nbr_far[NBR:, :] = nbr[NBR:, :]

        @pl.when(slab >= 0)
        def _():
            keep(turn + 1, own[...] + apply(lhs_node, nbr_far, 0, depth))

    local_sums(0)
    send_out(1, own_out[...])
    for copy in far_copies:
        copy.wait_recv()
    side = jnp.where(iota((8, E), 1) < PEER, 0, 2 * PEER)
    for face in range(6):
        at = slice(face * E, face * E + E)
        link = jnp.concatenate([far_arrived[way, face : face + 1, :] for way in range(2)], axis=1).astype(jnp.int32)
        turned = jnp.concatenate([far_arrived[way, 8 + face : 9 + face, :] for way in range(2)], axis=1)
        far_turn[face] = jnp.broadcast_to(turned.astype(jnp.int32), (8, E))
        row = jnp.where(link >= LOCAL, link - LOCAL + side[0:1, :], -1)
        wanted = jnp.broadcast_to(row, (4 * PEER, E))
        far_pick[:, at] = jnp.where(wanted == iota((4 * PEER, E), 0), 1.0, 0.0).astype(BF16)
    receive(0, None)
    update(0)
    local_sums(1, True)
    for side in range(2):
        relay(side).wait_recv()
    for at, part in enumerate((skip_arrived.at[0], send.at[0, 0], send.at[0, 1], skip_arrived.at[1])):
        for half in range(8):
            pair = split_pair(part[half * 8 : half * 8 + 8, :])
            far_table[half * 16 : half * 16 + 16, at * PEER : at * PEER + PEER] = jnp.concatenate(
                pair, axis=0
            ).astype(BF16)
    remote_part(far_pick, 0, far_turn, lambda: far_table[...], 4 * PEER)
    face_code = jnp.concatenate([far_arrived[way, 16:17, :] for way in range(2)], axis=1).astype(jnp.int32)
    added = face_traces(apply(lhs_node, nbr_far, 0, NBR), jnp.broadcast_to(face_code, (8, E)))
    for half, rows in enumerate(added):
        extra[0, half * 8 : half * 8 + 8, :] = rows[:, :PEER]
        extra[1, half * 8 : half * 8 + 8, :] = rows[:, PEER:]

    def advance(turn, top_later=False):
        depth = K if top_later else NBR
        if not top_later:
            local_sums(turn)
        receive(turn, top_later)
        remote_part(pick_near, 0, turn_out)
        if top_later:

            @pl.when(space >= 0)
            def _():
                own_out[...] += apply(lhs_node, nbr_far, 0, NBR)

            take_top(turn, True)

        @pl.when(slab >= 0)
        def _():
            begin, end = (NBR, K) if top_later else (0, NBR)
            send_out(turn + 1, own_out[...] + apply(lhs_node, nbr_far, begin, end))

        update(turn, depth)

    advance(1, True)

    @pl.loop(2, ROUNDS - 1)
    def _(turn):
        advance(turn)

    lhs_time[:E, :] = dot(by_time[...], lhs_node[:E, :]).astype(BF16)
    lhs_time[E:, :] = dot(by_time[...], lhs_node[E:, :]).astype(BF16)
    high, low = halves(const_node[...])
    const_time[...] = dot(by_time[...], high) + dot(by_time[...], low)
    own[...] = local_part(ROUNDS - 1, lhs_time, const_time)
    take_top(ROUNDS - 1)
    own[...] += apply(lhs_time, nbr, NBR, K)
    receive(ROUNDS - 1)
    remote_part(pick, LOCAL, turn_rows)

    @pl.when(slab >= 0)
    def _():
        out[0] = own[...] + apply(lhs_time, nbr_far, 0, NBR)

    for copy in space_copies(ROUNDS - 1) + far_copies + [relay(0), relay(1)]:
        copy.wait_send()

    @pl.when(slab < n_slab - 1)
    def _():
        top_copy(ROUNDS - 1).wait_send()


def body(n_space, n_slab, source, initial, inverse, lift, lift_time, links, orient, exports, counts):
    hbm = pl.BlockSpec(memory_space=pltpu.HBM)
    arrays = (source, initial, inverse, lift, lift_time.T, links, orient, exports.reshape(1, E))
    arrays = [pltpu.with_memory_space_constraint(array, pltpu.HBM) for array in arrays]
    vmem = pltpu.VMEM
    dma = pltpu.SemaphoreType.DMA
    state = pl.pallas_call(
        functools.partial(kernel, n_space, n_slab),
        name="window",
        out_shape=jax.ShapeDtypeStruct((1, 256, E), F32),
        in_specs=[hbm] * 8,
        out_specs=pl.BlockSpec(memory_space=pltpu.VMEM),
        scratch_shapes=[
            vmem((256, E), F32),
            vmem((64, E), F32),
            vmem((256, 256), F32),
            vmem((256, 384), F32),
            vmem((64, 256), F32),
            vmem((6, E), jnp.int32),
            vmem((6, E), jnp.int32),
            vmem((1, E), jnp.int32),
            vmem((TABLE, LOCAL), BF16),
            vmem((2 * PEER, LOCAL), BF16),
            vmem((128, TABLE), BF16),
            vmem((K, E), BF16),
            vmem((K, E), BF16),
            vmem((512, K), BF16),
            vmem((512, K), BF16),
            vmem((512, 256), BF16),
            vmem((256, E), F32),
            vmem((256, E), F32),
            vmem((256, 256), BF16),
            vmem((256, 256), BF16),
            vmem((256, E), F32),
            vmem((256, E), F32),
            vmem((256, 512), F32),
            vmem((512, K), BF16),
            vmem((16, LOCAL), jnp.int32),
            vmem((6, 8, E), jnp.int32),
            vmem((6, 8, E), jnp.int32),
            vmem((32, E), F32),
            vmem((E, E), BF16),
            vmem((64, 8, E), F32),
            vmem((2, 256, 128), F32),
            vmem((ROUNDS, 2, 64, PEER), F32),
            vmem((ROUNDS, 2, 64, PEER), F32),
            vmem((ROUNDS, 64, E), F32),
            vmem((ROUNDS, 64, E), F32),
            vmem((2, 24, PEER), F32),
            vmem((2, 24, PEER), F32),
            vmem((2, 64, PEER), F32),
            vmem((4 * PEER, LOCAL), BF16),
            vmem((128, 4 * PEER), BF16),
            vmem((6, 8, E), jnp.int32),
            vmem((2, 64, PEER), F32),
            dma((8,)),
            dma((2,)),
            dma((ROUNDS, 2)),
            dma,
            dma((ROUNDS,)),
            dma((2, 2)),
            dma((2, 2)),
        ],
        compiler_params=pltpu.CompilerParams(
            collective_id=0, has_side_effects=True, vmem_limit_bytes=48 * 1024 * 1024
        ),
    )(*arrays)
    live = jnp.arange(E, dtype=jnp.int32) < counts[0]
    return jnp.where(live[None, None, :], state, 0.0)


def solution(mesh):
    return jax.shard_map(
        functools.partial(body, mesh.shape["space"], mesh.shape["slab"]),
        mesh=mesh,
        in_specs=(
            P("slab", None, "space"),
            P(None, "space"),
            P(),
            P(),
            P(),
            P(None, "space"),
            P(None, "space"),
            P("space"),
            P("space"),
        ),
        out_specs=P("slab", None, "space"),
        check_vma=False,
    )
```

```python
import functools

import jax
import jax.numpy as jnp
from jax import lax
from jax.experimental import pallas as pl
from jax.experimental.pallas import tpu as pltpu
from jax.sharding import PartitionSpec as P

ROUNDS = 5
E = 256
PEER = 128
LOCAL = 6 * E
TABLE = LOCAL + 2 * PEER
NBR = 6 * 128
K = NBR + 128
F32 = jnp.float32
BF16 = jnp.bfloat16
HIGHEST = lax.Precision.HIGHEST
MESH = pl.DeviceIdType.MESH

FACES = (
    [(0, a, b) for a in range(4) for b in range(4)],
    [(3, a, b) for a in range(4) for b in range(4)],
    [(a, 0, b) for a in range(4) for b in range(4)],
    [(a, 3, b) for a in range(4) for b in range(4)],
    [(a, b, 0) for a in range(4) for b in range(4)],
    [(a, b, 3) for a in range(4) for b in range(4)],
)


def iota(shape, dim):
    return lax.broadcasted_iota(jnp.int32, shape, dim)


def dot(a, b):
    return jnp.dot(a, b, preferred_element_type=F32)


def halves(x):
    high = x.astype(BF16)
    return high, (x - high.astype(F32)).astype(BF16)


def split_pair(x):
    low = iota(x.shape, 0) < 4
    turned = pltpu.roll(x, 4, 0)
    tiles = []
    for d in (jnp.where(low, x, turned), jnp.where(low, turned, x)):
        rest = d - d.astype(BF16).astype(F32)
        tiles.append(jnp.where(low, d, rest))
    return tiles


def apply(lhs, rows, begin, end):
    parts = []
    for at in (0, 128):
        parts.append(
            dot(lhs[at : at + 128, begin:end], rows[begin:end, :])
            + dot(lhs[E + at : E + at + 128, begin:end], rows[begin:end, :])
        )
    return jnp.concatenate(parts, axis=0)


def oriented(block, code):
    swap = (code & 4) > 0
    back_a = (code & 1) > 0
    back_b = (code & 2) > 0
    four = range(4)
    v = [[block[(a * 4 + b) * 8 : (a * 4 + b) * 8 + 8, :] for b in four] for a in four]
    v = [[v[a][b] if a == b else jnp.where(swap, v[b][a], v[a][b]) for b in four] for a in four]
    v = [[jnp.where(back_a, v[3 - a][b], v[a][b]) for b in four] for a in four]
    v = [[jnp.where(back_b, v[a][3 - b], v[a][b]) for b in four] for a in four]
    return [v[a][b] for a in four for b in four]


def face_traces(state, code):
    low = iota(code.shape, 0) < 4

    def tile(node):
        return state[node * 4 : node * 4 + 8, :]

    rows = []
    for half in range(8):
        a, b = half // 2, 2 * (half % 2)
        near, far = a * 16 + b * 4, a * 16 + b * 4 + 4
        choices = [
            tile(a * 4 + b),
            tile(48 + a * 4 + b),
            tile(a * 16 + b),
            tile(a * 16 + 12 + b),
            jnp.where(low, tile(near), pltpu.roll(tile(far), 4, 0)),
            jnp.where(low, pltpu.roll(tile(near + 2), 4, 0), tile(far + 2)),
        ]
        value = choices[0]
        for face in range(1, 6):
            value = jnp.where(code == face, choices[face], value)
        rows.append(value)
    return rows


def kernel(
    n_space,
    n_slab,
    source,
    initial,
    inverse,
    lift,
    lift_time,
    links,
    orient,
    exports,
    out,
    v_source,
    v_initial,
    v_inverse,
    v_lift,
    v_lift_time,
    v_links,
    v_orient,
    v_exports,
    pick,
    pick_near,
    table,
    nbr,
    nbr_far,
    lhs_node,
    lhs_time,
    inv_node,
    const_node,
    const_time,
    by_node,
    by_time,
    own,
    own_out,
    face_out,
    nbr_near,
    lift_all,
    spread,
    link_rows,
    turn_rows,
    turn_out,
    codes,
    select,
    nodes,
    fresh,
    send,
    arrived,
    top_send,
    top_arrived,
    far_send,
    far_arrived,
    skip_arrived,
    far_pick,
    far_table,
    far_turn,
    extra,
    in_sem,
    send_sem,
    recv_sem,
    top_send_sem,
    top_recv_sem,
    far_sem,
    skip_sem,
):
    space = lax.axis_index("space")
    slab = lax.axis_index("slab")
    upper = {"space": lax.rem(space + 1, n_space)}
    lower = {"space": lax.rem(space + n_space - 1, n_space)}

    loads = []
    for at, (src, dst) in enumerate(
        (
            (exports, v_exports),
            (links, v_links),
            (orient, v_orient),
            (lift_time, v_lift_time),
            (initial, v_initial),
            (inverse, v_inverse),
            (source.at[0], v_source),
            (lift, v_lift),
        )
    ):
        copy = pltpu.make_async_copy(src, dst, in_sem.at[at])
        copy.start()
        loads.append(copy)

    barrier = pltpu.get_barrier_semaphore()
    for peer in (lower, upper):
        pl.semaphore_signal(barrier, inc=1, device_id=peer, device_id_type=MESH)

    @pl.when(slab > 0)
    def _():
        pl.semaphore_signal(barrier, inc=1, device_id={"slab": slab - 1}, device_id_type=MESH)

    @pl.when(slab < n_slab - 1)
    def _():
        pl.semaphore_signal(barrier, inc=1, device_id={"slab": slab + 1}, device_id_type=MESH)

    def space_copies(turn):
        return [
            pltpu.make_async_remote_copy(
                src_ref=send.at[turn, way],
                dst_ref=arrived.at[turn, 1 - way],
                send_sem=send_sem.at[way],
                recv_sem=recv_sem.at[turn, 1 - way],
                device_id=peer,
                device_id_type=MESH,
            )
            for way, peer in ((0, lower), (1, upper))
        ]

    def other_copies(source_of, target, sems, peers):
        return [
            pltpu.make_async_remote_copy(
                src_ref=source_of(way),
                dst_ref=target.at[1 - way],
                send_sem=sems.at[0, way],
                recv_sem=sems.at[1, 1 - way],
                device_id=peer,
                device_id_type=MESH,
            )
            for way, peer in enumerate(peers)
        ]

    far_copies = other_copies(lambda way: far_send.at[way], far_arrived, far_sem, (lower, upper))

    def first_arrival(side):
        return pltpu.make_async_remote_copy(
            src_ref=send.at[0, 1 - side],
            dst_ref=arrived.at[0, side],
            send_sem=send_sem.at[1 - side],
            recv_sem=recv_sem.at[0, side],
            device_id=lower,
            device_id_type=MESH,
        )

    def relay(side):
        return pltpu.make_async_remote_copy(
            src_ref=arrived.at[0, side],
            dst_ref=skip_arrived.at[side],
            send_sem=skip_sem.at[0, side],
            recv_sem=skip_sem.at[1, side],
            device_id={"space": lax.rem(space + n_space + 1 - 2 * side, n_space)},
            device_id_type=MESH,
        )

    near_side = lax.rem(space + 1, 2)

    def top_copy(turn):
        return pltpu.make_async_remote_copy(
            src_ref=top_send.at[turn],
            dst_ref=top_arrived.at[turn],
            send_sem=top_send_sem,
            recv_sem=top_recv_sem.at[turn],
            device_id={"slab": lax.rem(slab + 1, n_slab)},
            device_id_type=MESH,
        )

    def export_copy(turn, way):
        return pltpu.make_async_remote_copy(
            src_ref=send.at[turn, way],
            dst_ref=arrived.at[turn, 1 - way],
            send_sem=send_sem.at[way],
            recv_sem=recv_sem.at[turn, 1 - way],
            device_id={"space": lax.rem(space + n_space - 1 + 2 * way, n_space)},
            device_id_type=MESH,
        )

    def fill(turn, way, state):
        for half, rows in enumerate(face_traces(state, face_out[way])):
            send[turn, way, half * 8 : half * 8 + 8, :] = rows

    def send_one(turn, way, state):
        fill(turn, way, state)
        export_copy(turn - 1, way).wait_send()
        export_copy(turn, way).start()

    def keep(turn, state, turn_is_later=True):
        for half in range(2):
            fresh[half] = state[:, half * 128 : half * 128 + 128]
        for half in range(2):
            top_send[turn, :, half * 128 : half * 128 + 128] = fresh[half, pl.ds(3, 64, stride=4), :]
        if not turn_is_later:
            return

        @pl.when(slab < n_slab - 1)
        def _():
            top_copy(turn - 1).wait_send()
            top_copy(turn).start()

    def exported(state):
        high, low = halves(state)
        return dot(high, select[...]) + dot(low, select[...])

    row, column = iota((E, E), 0), iota((E, E), 1)
    by_node[...] = jnp.where(column == (row & 3) * 64 + (row >> 2), 1.0, 0.0).astype(BF16)
    by_time[...] = jnp.where(column == (row & 63) * 4 + (row >> 6), 1.0, 0.0).astype(BF16)
    column = iota((512, K), 1)
    face_source = ((column & 3) * 16 + ((column >> 3) & 15)) * 6 + (column >> 7)
    wanted_row = jnp.where(column < NBR, face_source, 384 + (column & 63))
    spread[...] = jnp.where(iota((512, K), 0) == wanted_row, 1.0, 0.0).astype(BF16)
    codes[...] = jnp.zeros((32, E), F32)
    nbr[NBR:, :] = jnp.zeros((128, E), BF16)
    nbr_far[NBR:, :] = jnp.zeros((128, E), BF16)
    lift_all[:, 384:] = jnp.zeros((E, 128), F32)

    for load in loads[:6]:
        load.wait()
    element = jnp.broadcast_to(v_exports[...] & 255, (E, E))
    select[...] = jnp.where(element == iota((E, E), 0), 1.0, 0.0).astype(BF16)
    codes[0:6, :] = (v_links[...] >> 8).astype(F32)
    codes[8:14, :] = (v_links[...] & 255).astype(F32)
    codes[16:22, :] = v_orient[...].astype(F32)
    codes[24:25, :] = (v_exports[...] >> 8).astype(F32)
    moved = dot(codes[0:24, :].astype(BF16), select[...])
    time_high, time_low = halves(v_lift_time[...].T)
    first_high, first_low = halves(v_initial[...])
    start = dot(time_high, first_high) + dot(time_high, first_low) + dot(time_low, first_high)
    inv_high, inv_low = halves(v_inverse[...])
    inv_node[:E, :] = dot(by_node[...], inv_high).astype(BF16)
    inv_node[E:, :] = dot(by_node[...], inv_low).astype(BF16)
    out_link = moved[0:8, :] * 256.0 + moved[8:16, :]
    for way in range(2):
        at = slice(way * PEER, way * PEER + PEER)
        far_send[way, 0:8, :] = out_link[:, at]
        far_send[way, 8:16, :] = moved[16:24, at]
        far_send[way, 16:24, :] = codes[24:32, at]
    loads[6].wait()
    rhs_high, rhs_low = halves(v_source[...] + jnp.where(slab == 0, start, 0.0))
    first = dot(inv_node[:E, :], rhs_high) + dot(inv_node[:E, :], rhs_low) + dot(inv_node[E:, :], rhs_high)
    const_node[...] = first
    leaving = exported(first)
    keep(0, first, False)
    for way in range(2):
        half = slice(way * PEER, way * PEER + PEER)
        face_out[way] = jnp.broadcast_to(v_exports[:, half] >> 8, (8, PEER))
        fill(0, way, leaving[:, half])
    count = jnp.where(slab > 0, 1, 0) + jnp.where(slab < n_slab - 1, 1, 0) + 2
    pl.semaphore_wait(barrier, count)
    for copy in space_copies(0):
        copy.start()

    @pl.when(slab < n_slab - 1)
    def _():
        top_copy(0).start()

    for copy in far_copies:
        copy.start()

    turn_out_rows = moved[16:24, :].astype(jnp.int32)
    loads[7].wait()
    lift_all[:, :384] = v_lift[...]
    lift_all[:, 384:448] = v_lift_time[...].T
    lift_high, lift_low = halves(lift_all[...])
    node_high, node_low = halves(
        dot(inv_node[:E, :], lift_high) + dot(inv_node[:E, :], lift_low) + dot(inv_node[E:, :], lift_high)
    )
    for face in range(6):
        at = slice(face * E, face * E + E)
        link_rows[:, at] = jnp.broadcast_to(v_links[face : face + 1, :], (16, E))
        turn_rows[face] = jnp.broadcast_to(v_orient[face : face + 1, :], (8, E))
        wanted = jnp.broadcast_to(out_link[face : face + 1, :].astype(jnp.int32), (2 * PEER, E))
        hit = jnp.where(wanted == iota((2 * PEER, E), 0) + LOCAL, 1.0, 0.0).astype(BF16)
        code = jnp.broadcast_to(turn_out_rows[face : face + 1, :], (8, E))
        for way in range(2):
            half = slice(way * PEER, way * PEER + PEER)
            pick_near[way, :, face * PEER : face * PEER + PEER] = hit[:, half]
            turn_out[way, face] = code[:, half]
    one, zero = jnp.ones((16, E), BF16), jnp.zeros((16, E), BF16)
    for face in range(6):
        at = slice(face * E, face * E + E)
        for tile in range(TABLE // E):
            link = link_rows[:, at]
            keys = jnp.where(link >> 8 == tile, link & 255, -1).astype(F32).astype(BF16)
            for step in range(E // 16):
                row = (iota((16, E), 0) + step * 16).astype(F32).astype(BF16)
                base = tile * E + step * 16
                pick[base : base + 16, at] = jnp.where(keys == row, one, zero)
    lhs_node[:E, :] = dot(node_high, spread[...]).astype(BF16)
    lhs_node[E:, :] = dot(node_low, spread[...]).astype(BF16)
    first_arrival(near_side).wait_recv()
    relay(near_side).start()

    def local_part(turn, lhs, const):
        for pair in range(32):
            for half in range(2):
                at = slice(half * 128, half * 128 + 128)
                one, two = split_pair(fresh[half, pair * 8 : pair * 8 + 8, :])
                nodes[2 * pair, :, at] = one
                nodes[2 * pair + 1, :, at] = two
        for face, members in enumerate(FACES):
            for half in range(8):
                rows = [nodes[i * 16 + j * 4 + k] for i, j, k in members[2 * half : 2 * half + 2]]
                table[half * 16 : half * 16 + 16, face * E : face * E + E] = jnp.concatenate(
                    rows, axis=0
                ).astype(BF16)
        for face in range(6):
            at = slice(face * E, face * E + E)
            store_rows(nbr, face, oriented(dot(table[:, :LOCAL], pick[:LOCAL, at]), turn_rows[face]))
        return const[...] + apply(lhs, nbr, 0, NBR)

    def take_top(turn, for_exports=False):
        @pl.when(slab > 0)
        def _():
            top_copy(turn).wait_recv()
            high, low = halves(top_arrived[turn])
            nbr[NBR : NBR + 64, :] = high
            nbr[NBR + 64 :, :] = low
            if for_exports:
                nbr_far[NBR:, :] = dot(nbr[NBR:, :], select[...]).astype(BF16)

    def store_rows(ref, face, tiles):
        for half in range(8):
            row = face * 128 + half * 16
            ref[row : row + 16, :] = jnp.concatenate(tiles[2 * half : 2 * half + 2], axis=0).astype(BF16)

    def receive(turn, completed=False):
        if completed is None:
            first_arrival(1 - near_side).wait_recv()
            relay(1 - near_side).start()
        else:
            for copy in space_copies(turn):
                copy.wait_recv()
        for way in range(2):
            for half in range(8):
                rows = slice(half * 8, half * 8 + 8)
                value = arrived[turn, way, rows, :]
                pair = split_pair(value + extra[way, rows, :] if completed else value)
                table[
                    half * 16 : half * 16 + 16, LOCAL + way * PEER : LOCAL + way * PEER + PEER
                ] = jnp.concatenate(pair, axis=0).astype(BF16)

    def remote_part(chosen, base, turns, columns=lambda: table[:, LOCAL:], depth=2 * PEER):
        for face in (0, 2, 4):
            block = dot(columns(), chosen[base : base + depth, face * E : face * E + 2 * E])
            store_rows(nbr_far, face, oriented(block[:, :E], turns[face]))
            store_rows(nbr_far, face + 1, oriented(block[:, E:], turns[face + 1]))


    def local_sums(turn, top_later=False):
        so_far = local_part(turn, lhs_node, const_node)
        if not top_later:
            take_top(turn)
            so_far += apply(lhs_node, nbr, NBR, K)
        own[...] = so_far
        leaving = exported(so_far)
        own_out[0] = leaving[:, :PEER]
        own_out[1] = leaving[:, PEER:]

    def update(turn, depth=NBR):
        @pl.when(space >= 0)
        def _():
            remote_part(pick, LOCAL, turn_rows)
            if depth > NBR:
                nbr_far[NBR:, :] = nbr[NBR:, :]

        @pl.when(slab >= 0)
        def _():
            keep(turn + 1, own[...] + apply(lhs_node, nbr_far, 0, depth))

    local_sums(0)
    for way in range(2):
        send_one(1, way, own_out[way])
    for copy in far_copies:
        copy.wait_recv()
    side = jnp.where(iota((8, E), 1) < PEER, 0, 2 * PEER)
    for face in range(6):
        at = slice(face * E, face * E + E)
        link = jnp.concatenate([far_arrived[way, face : face + 1, :] for way in range(2)], axis=1).astype(jnp.int32)
        turned = jnp.concatenate([far_arrived[way, 8 + face : 9 + face, :] for way in range(2)], axis=1)
        far_turn[face] = jnp.broadcast_to(turned.astype(jnp.int32), (8, E))
        row = jnp.where(link >= LOCAL, link - LOCAL + side[0:1, :], -1)
        wanted = jnp.broadcast_to(row, (4 * PEER, E))
        far_pick[:, at] = jnp.where(wanted == iota((4 * PEER, E), 0), 1.0, 0.0).astype(BF16)
    receive(0, None)
    update(0)
    local_sums(1, True)
    for side in range(2):
        relay(side).wait_recv()
    for at, part in enumerate((skip_arrived.at[0], send.at[0, 0], send.at[0, 1], skip_arrived.at[1])):
        for half in range(8):
            pair = split_pair(part[half * 8 : half * 8 + 8, :])
            far_table[half * 16 : half * 16 + 16, at * PEER : at * PEER + PEER] = jnp.concatenate(
                pair, axis=0
            ).astype(BF16)
    remote_part(far_pick, 0, far_turn, lambda: far_table[...], 4 * PEER)
    face_code = jnp.concatenate([far_arrived[way, 16:17, :] for way in range(2)], axis=1).astype(jnp.int32)
    added = face_traces(apply(lhs_node, nbr_far, 0, NBR), jnp.broadcast_to(face_code, (8, E)))
    for half, rows in enumerate(added):
        extra[0, half * 8 : half * 8 + 8, :] = rows[:, :PEER]
        extra[1, half * 8 : half * 8 + 8, :] = rows[:, PEER:]

    def near_part(way):
        block = dot(table[:, LOCAL:], pick_near[way])
        for face in range(6):
            store_rows(nbr_near, face, oriented(block[:, face * PEER : face * PEER + PEER], turn_out[way, face]))

    def advance(turn, top_later=False):
        depth = K if top_later else NBR
        if not top_later:
            local_sums(turn)
        receive(turn, top_later)
        far_side = 1 - near_side
        near_part(far_side)
        if top_later:

            @pl.when(space >= 0)
            def _():
                own_out[far_side] = own_out[far_side] + apply(lhs_node, nbr_near, 0, NBR)

            take_top(turn, True)

        @pl.when(slab >= 0)
        def _():
            if top_later:
                late = apply(lhs_node, nbr_far, NBR, K)
                own_out[0] = own_out[0] + late[:, :PEER]
                own_out[1] = own_out[1] + late[:, PEER:]
                send_one(turn + 1, far_side, own_out[far_side])
            else:
                send_one(turn + 1, far_side, own_out[far_side] + apply(lhs_node, nbr_near, 0, NBR))

        update(turn, depth)

        @pl.when(space >= 0)
        def _():
            near_part(near_side)

        @pl.when(slab >= 0)
        def _():
            send_one(turn + 1, near_side, own_out[near_side] + apply(lhs_node, nbr_near, 0, NBR))

    advance(1, True)

    @pl.loop(2, ROUNDS - 1)
    def _(turn):
        advance(turn)

    lhs_time[:E, :] = dot(by_time[...], lhs_node[:E, :]).astype(BF16)
    lhs_time[E:, :] = dot(by_time[...], lhs_node[E:, :]).astype(BF16)
    high, low = halves(const_node[...])
    const_time[...] = dot(by_time[...], high) + dot(by_time[...], low)
    own[...] = local_part(ROUNDS - 1, lhs_time, const_time)
    take_top(ROUNDS - 1)
    own[...] += apply(lhs_time, nbr, NBR, K)
    receive(ROUNDS - 1)
    remote_part(pick, LOCAL, turn_rows)

    @pl.when(slab >= 0)
    def _():
        out[0] = own[...] + apply(lhs_time, nbr_far, 0, NBR)

    for copy in space_copies(ROUNDS - 1) + far_copies + [relay(0), relay(1)]:
        copy.wait_send()

    @pl.when(slab < n_slab - 1)
    def _():
        top_copy(ROUNDS - 1).wait_send()


def body(n_space, n_slab, source, initial, inverse, lift, lift_time, links, orient, exports, counts):
    hbm = pl.BlockSpec(memory_space=pltpu.HBM)
    arrays = (source, initial, inverse, lift, lift_time.T, links, orient, exports.reshape(1, E))
    arrays = [pltpu.with_memory_space_constraint(array, pltpu.HBM) for array in arrays]
    vmem = pltpu.VMEM
    dma = pltpu.SemaphoreType.DMA
    state = pl.pallas_call(
        functools.partial(kernel, n_space, n_slab),
        name="window",
        out_shape=jax.ShapeDtypeStruct((1, 256, E), F32),
        in_specs=[hbm] * 8,
        out_specs=pl.BlockSpec(memory_space=pltpu.VMEM),
        scratch_shapes=[
            vmem((256, E), F32),
            vmem((64, E), F32),
            vmem((256, 256), F32),
            vmem((256, 384), F32),
            vmem((64, 256), F32),
            vmem((6, E), jnp.int32),
            vmem((6, E), jnp.int32),
            vmem((1, E), jnp.int32),
            vmem((TABLE, LOCAL), BF16),
            vmem((2, 2 * PEER, 6 * PEER), BF16),
            vmem((128, TABLE), BF16),
            vmem((K, E), BF16),
            vmem((K, E), BF16),
            vmem((512, K), BF16),
            vmem((512, K), BF16),
            vmem((512, 256), BF16),
            vmem((256, E), F32),
            vmem((256, E), F32),
            vmem((256, 256), BF16),
            vmem((256, 256), BF16),
            vmem((256, E), F32),
            vmem((2, 256, PEER), F32),
            vmem((2, 8, PEER), jnp.int32),
            vmem((NBR, PEER), BF16),
            vmem((256, 512), F32),
            vmem((512, K), BF16),
            vmem((16, LOCAL), jnp.int32),
            vmem((6, 8, E), jnp.int32),
            vmem((2, 6, 8, PEER), jnp.int32),
            vmem((32, E), F32),
            vmem((E, E), BF16),
            vmem((64, 8, E), F32),
            vmem((2, 256, 128), F32),
            vmem((ROUNDS, 2, 64, PEER), F32),
            vmem((ROUNDS, 2, 64, PEER), F32),
            vmem((ROUNDS, 64, E), F32),
            vmem((ROUNDS, 64, E), F32),
            vmem((2, 24, PEER), F32),
            vmem((2, 24, PEER), F32),
            vmem((2, 64, PEER), F32),
            vmem((4 * PEER, LOCAL), BF16),
            vmem((128, 4 * PEER), BF16),
            vmem((6, 8, E), jnp.int32),
            vmem((2, 64, PEER), F32),
            dma((8,)),
            dma((2,)),
            dma((ROUNDS, 2)),
            dma,
            dma((ROUNDS,)),
            dma((2, 2)),
            dma((2, 2)),
        ],
        compiler_params=pltpu.CompilerParams(
            collective_id=0, has_side_effects=True, vmem_limit_bytes=48 * 1024 * 1024
        ),
    )(*arrays)
    live = jnp.arange(E, dtype=jnp.int32) < counts[0]
    return jnp.where(live[None, None, :], state, 0.0)


def solution(mesh):
    return jax.shard_map(
        functools.partial(body, mesh.shape["space"], mesh.shape["slab"]),
        mesh=mesh,
        in_specs=(
            P("slab", None, "space"),
            P(None, "space"),
            P(),
            P(),
            P(),
            P(None, "space"),
            P(None, "space"),
            P("space"),
            P("space"),
        ),
        out_specs=P("slab", None, "space"),
        check_vma=False,
    )
```

```python
import functools

import jax
import jax.numpy as jnp
from jax import lax
from jax.experimental import pallas as pl
from jax.experimental.pallas import tpu as pltpu
from jax.sharding import PartitionSpec as P

ROUNDS = 5
E = 256
PEER = 128
LOCAL = 6 * E
TABLE = LOCAL + 2 * PEER
NBR = 6 * 128
K = NBR + 128
F32 = jnp.float32
BF16 = jnp.bfloat16
HIGHEST = lax.Precision.HIGHEST
MESH = pl.DeviceIdType.MESH

FACES = (
    [(0, a, b) for a in range(4) for b in range(4)],
    [(3, a, b) for a in range(4) for b in range(4)],
    [(a, 0, b) for a in range(4) for b in range(4)],
    [(a, 3, b) for a in range(4) for b in range(4)],
    [(a, b, 0) for a in range(4) for b in range(4)],
    [(a, b, 3) for a in range(4) for b in range(4)],
)


def iota(shape, dim):
    return lax.broadcasted_iota(jnp.int32, shape, dim)


def dot(a, b):
    return jnp.dot(a, b, preferred_element_type=F32)


def halves(x):
    high = x.astype(BF16)
    return high, (x - high.astype(F32)).astype(BF16)


def split_pair(x):
    low = iota(x.shape, 0) < 4
    turned = pltpu.roll(x, 4, 0)
    tiles = []
    for d in (jnp.where(low, x, turned), jnp.where(low, turned, x)):
        rest = d - d.astype(BF16).astype(F32)
        tiles.append(jnp.where(low, d, rest))
    return tiles


def apply(lhs, rows, begin, end):
    parts = []
    for at in (0, 128):
        parts.append(
            dot(lhs[at : at + 128, begin:end], rows[begin:end, :])
            + dot(lhs[E + at : E + at + 128, begin:end], rows[begin:end, :])
        )
    return jnp.concatenate(parts, axis=0)


def oriented(block, code):
    swap = (code & 4) > 0
    back_a = (code & 1) > 0
    back_b = (code & 2) > 0
    four = range(4)
    v = [[block[(a * 4 + b) * 8 : (a * 4 + b) * 8 + 8, :] for b in four] for a in four]
    v = [[v[a][b] if a == b else jnp.where(swap, v[b][a], v[a][b]) for b in four] for a in four]
    v = [[jnp.where(back_a, v[3 - a][b], v[a][b]) for b in four] for a in four]
    v = [[jnp.where(back_b, v[a][3 - b], v[a][b]) for b in four] for a in four]
    return [v[a][b] for a in four for b in four]


def face_traces(state, code):
    low = iota(code.shape, 0) < 4

    def tile(node):
        return state[node * 4 : node * 4 + 8, :]

    rows = []
    for half in range(8):
        a, b = half // 2, 2 * (half % 2)
        near, far = a * 16 + b * 4, a * 16 + b * 4 + 4
        choices = [
            tile(a * 4 + b),
            tile(48 + a * 4 + b),
            tile(a * 16 + b),
            tile(a * 16 + 12 + b),
            jnp.where(low, tile(near), pltpu.roll(tile(far), 4, 0)),
            jnp.where(low, pltpu.roll(tile(near + 2), 4, 0), tile(far + 2)),
        ]
        value = choices[0]
        for face in range(1, 6):
            value = jnp.where(code == face, choices[face], value)
        rows.append(value)
    return rows


def kernel(
    n_space,
    n_slab,
    source,
    initial,
    inverse,
    lift,
    lift_time,
    links,
    orient,
    exports,
    out,
    v_source,
    v_initial,
    v_inverse,
    v_lift,
    v_lift_time,
    v_links,
    v_orient,
    v_exports,
    pick,
    pick_near,
    table,
    nbr,
    nbr_far,
    lhs_node,
    lhs_time,
    inv_node,
    const_node,
    const_time,
    by_node,
    by_time,
    own,
    own_out,
    face_out,
    nbr_near,
    lift_all,
    spread,
    link_rows,
    turn_rows,
    turn_out,
    codes,
    select,
    nodes,
    fresh,
    send,
    arrived,
    top_send,
    top_arrived,
    far_send,
    far_arrived,
    skip_arrived,
    far_pick,
    far_table,
    far_turn,
    extra,
    in_sem,
    send_sem,
    recv_sem,
    top_send_sem,
    top_recv_sem,
    far_sem,
    skip_sem,
):
    space = lax.axis_index("space")
    slab = lax.axis_index("slab")
    upper = {"space": lax.rem(space + 1, n_space)}
    lower = {"space": lax.rem(space + n_space - 1, n_space)}

    barrier = pltpu.get_barrier_semaphore()
    for peer in (lower, upper):
        pl.semaphore_signal(barrier, inc=1, device_id=peer, device_id_type=MESH)

    @pl.when(slab > 0)
    def _():
        pl.semaphore_signal(barrier, inc=1, device_id={"slab": slab - 1}, device_id_type=MESH)

    @pl.when(slab < n_slab - 1)
    def _():
        pl.semaphore_signal(barrier, inc=1, device_id={"slab": slab + 1}, device_id_type=MESH)

    loads = []
    for at, (src, dst) in enumerate(
        (
            (exports, v_exports),
            (links, v_links),
            (orient, v_orient),
            (lift_time, v_lift_time),
            (initial, v_initial),
            (inverse, v_inverse),
            (source.at[0], v_source),
            (lift, v_lift),
        )
    ):
        copy = pltpu.make_async_copy(src, dst, in_sem.at[at])
        copy.start()
        loads.append(copy)

    def space_copies(turn):
        return [
            pltpu.make_async_remote_copy(
                src_ref=send.at[turn, way],
                dst_ref=arrived.at[turn, 1 - way],
                send_sem=send_sem.at[way],
                recv_sem=recv_sem.at[turn, 1 - way],
                device_id=peer,
                device_id_type=MESH,
            )
            for way, peer in ((0, lower), (1, upper))
        ]

    def other_copies(source_of, target, sems, peers):
        return [
            pltpu.make_async_remote_copy(
                src_ref=source_of(way),
                dst_ref=target.at[1 - way],
                send_sem=sems.at[0, way],
                recv_sem=sems.at[1, 1 - way],
                device_id=peer,
                device_id_type=MESH,
            )
            for way, peer in enumerate(peers)
        ]

    far_copies = other_copies(lambda way: far_send.at[way], far_arrived, far_sem, (lower, upper))

    def first_arrival(side):
        return pltpu.make_async_remote_copy(
            src_ref=send.at[0, 1 - side],
            dst_ref=arrived.at[0, side],
            send_sem=send_sem.at[1 - side],
            recv_sem=recv_sem.at[0, side],
            device_id=lower,
            device_id_type=MESH,
        )

    def relay(side):
        return pltpu.make_async_remote_copy(
            src_ref=arrived.at[0, side],
            dst_ref=skip_arrived.at[side],
            send_sem=skip_sem.at[0, side],
            recv_sem=skip_sem.at[1, side],
            device_id={"space": lax.rem(space + n_space + 1 - 2 * side, n_space)},
            device_id_type=MESH,
        )

    near_side = lax.rem(space + 1, 2)

    def top_copy(turn):
        return pltpu.make_async_remote_copy(
            src_ref=top_send.at[turn],
            dst_ref=top_arrived.at[turn],
            send_sem=top_send_sem,
            recv_sem=top_recv_sem.at[turn],
            device_id={"slab": lax.rem(slab + 1, n_slab)},
            device_id_type=MESH,
        )

    def export_copy(turn, way):
        return pltpu.make_async_remote_copy(
            src_ref=send.at[turn, way],
            dst_ref=arrived.at[turn, 1 - way],
            send_sem=send_sem.at[way],
            recv_sem=recv_sem.at[turn, 1 - way],
            device_id={"space": lax.rem(space + n_space - 1 + 2 * way, n_space)},
            device_id_type=MESH,
        )

    def fill(turn, way, state):
        for half, rows in enumerate(face_traces(state, face_out[way])):
            send[turn, way, half * 8 : half * 8 + 8, :] = rows

    def send_one(turn, way, state):
        fill(turn, way, state)
        export_copy(turn - 1, way).wait_send()
        export_copy(turn, way).start()

    def keep(turn, state, turn_is_later=True):
        for half in range(2):
            fresh[half] = state[:, half * 128 : half * 128 + 128]
        for half in range(2):
            top_send[turn, :, half * 128 : half * 128 + 128] = fresh[half, pl.ds(3, 64, stride=4), :]
        if not turn_is_later:
            return

        @pl.when(slab < n_slab - 1)
        def _():
            top_copy(turn - 1).wait_send()
            top_copy(turn).start()

    def exported(state):
        high, low = halves(state)
        return dot(high, select[...]) + dot(low, select[...])

    row, column = iota((E, E), 0), iota((E, E), 1)
    by_node[...] = jnp.where(column == (row & 3) * 64 + (row >> 2), 1.0, 0.0).astype(BF16)
    by_time[...] = jnp.where(column == (row & 63) * 4 + (row >> 6), 1.0, 0.0).astype(BF16)
    column = iota((512, K), 1)
    face_source = ((column & 3) * 16 + ((column >> 3) & 15)) * 6 + (column >> 7)
    wanted_row = jnp.where(column < NBR, face_source, 384 + (column & 63))
    spread[...] = jnp.where(iota((512, K), 0) == wanted_row, 1.0, 0.0).astype(BF16)
    codes[...] = jnp.zeros((32, E), F32)
    nbr[NBR:, :] = jnp.zeros((128, E), BF16)
    nbr_far[NBR:, :] = jnp.zeros((128, E), BF16)
    lift_all[:, 384:] = jnp.zeros((E, 128), F32)

    for load in loads[:5]:
        load.wait()
    element = jnp.broadcast_to(v_exports[...] & 255, (E, E))
    select[...] = jnp.where(element == iota((E, E), 0), 1.0, 0.0).astype(BF16)
    codes[0:6, :] = (v_links[...] >> 8).astype(F32)
    codes[8:14, :] = (v_links[...] & 255).astype(F32)
    codes[16:22, :] = v_orient[...].astype(F32)
    codes[24:25, :] = (v_exports[...] >> 8).astype(F32)
    moved = dot(codes[0:24, :].astype(BF16), select[...])
    time_high, time_low = halves(v_lift_time[...].T)
    first_high, first_low = halves(v_initial[...])
    start = dot(time_high, first_high) + dot(time_high, first_low) + dot(time_low, first_high)
    loads[5].wait()
    inv_high, inv_low = halves(v_inverse[...])
    inv_node[:E, :] = dot(by_node[...], inv_high).astype(BF16)
    inv_node[E:, :] = dot(by_node[...], inv_low).astype(BF16)
    out_link = moved[0:8, :] * 256.0 + moved[8:16, :]
    for way in range(2):
        at = slice(way * PEER, way * PEER + PEER)
        far_send[way, 0:8, :] = out_link[:, at]
        far_send[way, 8:16, :] = moved[16:24, at]
        far_send[way, 16:24, :] = codes[24:32, at]
    loads[6].wait()
    rhs_high, rhs_low = halves(v_source[...] + jnp.where(slab == 0, start, 0.0))
    first = dot(inv_node[:E, :], rhs_high) + dot(inv_node[:E, :], rhs_low) + dot(inv_node[E:, :], rhs_high)
    const_node[...] = first
    leaving = exported(first)
    keep(0, first, False)
    for way in range(2):
        half = slice(way * PEER, way * PEER + PEER)
        face_out[way] = jnp.broadcast_to(v_exports[:, half] >> 8, (8, PEER))
        fill(0, way, leaving[:, half])
    count = jnp.where(slab > 0, 1, 0) + jnp.where(slab < n_slab - 1, 1, 0) + 2
    pl.semaphore_wait(barrier, count)
    for copy in space_copies(0):
        copy.start()

    @pl.when(slab < n_slab - 1)
    def _():
        top_copy(0).start()

    for copy in far_copies:
        copy.start()

    turn_out_rows = moved[16:24, :].astype(jnp.int32)
    loads[7].wait()
    lift_all[:, :384] = v_lift[...]
    lift_all[:, 384:448] = v_lift_time[...].T
    lift_high, lift_low = halves(lift_all[...])
    node_high, node_low = halves(
        dot(inv_node[:E, :], lift_high) + dot(inv_node[:E, :], lift_low) + dot(inv_node[E:, :], lift_high)
    )
    for face in range(6):
        at = slice(face * E, face * E + E)
        link_rows[:, at] = jnp.broadcast_to(v_links[face : face + 1, :], (16, E))
        turn_rows[face] = jnp.broadcast_to(v_orient[face : face + 1, :], (8, E))
        wanted = jnp.broadcast_to(out_link[face : face + 1, :].astype(jnp.int32), (2 * PEER, E))
        hit = jnp.where(wanted == iota((2 * PEER, E), 0) + LOCAL, 1.0, 0.0).astype(BF16)
        code = jnp.broadcast_to(turn_out_rows[face : face + 1, :], (8, E))
        for way in range(2):
            half = slice(way * PEER, way * PEER + PEER)
            pick_near[way, :, face * PEER : face * PEER + PEER] = hit[:, half]
            turn_out[way, face] = code[:, half]
    one, zero = jnp.ones((16, E), BF16), jnp.zeros((16, E), BF16)
    for face in range(6):
        at = slice(face * E, face * E + E)
        for tile in range(TABLE // E):
            link = link_rows[:, at]
            keys = jnp.where(link >> 8 == tile, link & 255, -1).astype(F32).astype(BF16)
            for step in range(E // 16):
                row = (iota((16, E), 0) + step * 16).astype(F32).astype(BF16)
                base = tile * E + step * 16
                pick[base : base + 16, at] = jnp.where(keys == row, one, zero)
    lhs_node[:E, :] = dot(node_high, spread[...]).astype(BF16)
    lhs_node[E:, :] = dot(node_low, spread[...]).astype(BF16)
    first_arrival(near_side).wait_recv()
    relay(near_side).start()

    def local_part(turn, lhs, const):
        for pair in range(32):
            for half in range(2):
                at = slice(half * 128, half * 128 + 128)
                one, two = split_pair(fresh[half, pair * 8 : pair * 8 + 8, :])
                nodes[2 * pair, :, at] = one
                nodes[2 * pair + 1, :, at] = two
        for face, members in enumerate(FACES):
            for half in range(8):
                rows = [nodes[i * 16 + j * 4 + k] for i, j, k in members[2 * half : 2 * half + 2]]
                table[half * 16 : half * 16 + 16, face * E : face * E + E] = jnp.concatenate(
                    rows, axis=0
                ).astype(BF16)
        for face in range(6):
            at = slice(face * E, face * E + E)
            store_rows(nbr, face, oriented(dot(table[:, :LOCAL], pick[:LOCAL, at]), turn_rows[face]))
        return const[...] + apply(lhs, nbr, 0, NBR)

    def take_top(turn, for_exports=False):
        @pl.when(slab > 0)
        def _():
            top_copy(turn).wait_recv()
            high, low = halves(top_arrived[turn])
            nbr[NBR : NBR + 64, :] = high
            nbr[NBR + 64 :, :] = low
            if for_exports:
                nbr_far[NBR:, :] = dot(nbr[NBR:, :], select[...]).astype(BF16)

    def store_rows(ref, face, tiles):
        for half in range(8):
            row = face * 128 + half * 16
            ref[row : row + 16, :] = jnp.concatenate(tiles[2 * half : 2 * half + 2], axis=0).astype(BF16)

    def receive(turn, completed=False):
        if completed is None:
            first_arrival(1 - near_side).wait_recv()
            relay(1 - near_side).start()
        else:
            for copy in space_copies(turn):
                copy.wait_recv()
        for way in range(2):
            for half in range(8):
                rows = slice(half * 8, half * 8 + 8)
                value = arrived[turn, way, rows, :]
                pair = split_pair(value + extra[way, rows, :] if completed else value)
                table[
                    half * 16 : half * 16 + 16, LOCAL + way * PEER : LOCAL + way * PEER + PEER
                ] = jnp.concatenate(pair, axis=0).astype(BF16)

    def remote_part(chosen, base, turns, columns=lambda: table[:, LOCAL:], depth=2 * PEER):
        for face in (0, 2, 4):
            block = dot(columns(), chosen[base : base + depth, face * E : face * E + 2 * E])
            store_rows(nbr_far, face, oriented(block[:, :E], turns[face]))
            store_rows(nbr_far, face + 1, oriented(block[:, E:], turns[face + 1]))


    def local_sums(turn, top_later=False):
        so_far = local_part(turn, lhs_node, const_node)
        if not top_later:
            take_top(turn)
            so_far += apply(lhs_node, nbr, NBR, K)
        own[...] = so_far
        leaving = exported(so_far)
        own_out[0] = leaving[:, :PEER]
        own_out[1] = leaving[:, PEER:]

    def update(turn, depth=NBR):
        @pl.when(space >= 0)
        def _():
            remote_part(pick, LOCAL, turn_rows)
            if depth > NBR:
                nbr_far[NBR:, :] = nbr[NBR:, :]

        @pl.when(slab >= 0)
        def _():
            keep(turn + 1, own[...] + apply(lhs_node, nbr_far, 0, depth))

    local_sums(0)
    for way in range(2):
        send_one(1, way, own_out[way])
    for copy in far_copies:
        copy.wait_recv()
    side = jnp.where(iota((8, E), 1) < PEER, 0, 2 * PEER)
    for face in range(6):
        at = slice(face * E, face * E + E)
        link = jnp.concatenate([far_arrived[way, face : face + 1, :] for way in range(2)], axis=1).astype(jnp.int32)
        turned = jnp.concatenate([far_arrived[way, 8 + face : 9 + face, :] for way in range(2)], axis=1)
        far_turn[face] = jnp.broadcast_to(turned.astype(jnp.int32), (8, E))
        row = jnp.where(link >= LOCAL, link - LOCAL + side[0:1, :], -1)
        wanted = jnp.broadcast_to(row, (4 * PEER, E))
        far_pick[:, at] = jnp.where(wanted == iota((4 * PEER, E), 0), 1.0, 0.0).astype(BF16)
    receive(0, None)
    update(0)
    local_sums(1, True)
    for side in range(2):
        relay(side).wait_recv()
    for at, part in enumerate((skip_arrived.at[0], send.at[0, 0], send.at[0, 1], skip_arrived.at[1])):
        for half in range(8):
            pair = split_pair(part[half * 8 : half * 8 + 8, :])
            far_table[half * 16 : half * 16 + 16, at * PEER : at * PEER + PEER] = jnp.concatenate(
                pair, axis=0
            ).astype(BF16)
    remote_part(far_pick, 0, far_turn, lambda: far_table[...], 4 * PEER)
    face_code = jnp.concatenate([far_arrived[way, 16:17, :] for way in range(2)], axis=1).astype(jnp.int32)
    added = face_traces(apply(lhs_node, nbr_far, 0, NBR), jnp.broadcast_to(face_code, (8, E)))
    for half, rows in enumerate(added):
        extra[0, half * 8 : half * 8 + 8, :] = rows[:, :PEER]
        extra[1, half * 8 : half * 8 + 8, :] = rows[:, PEER:]

    def near_part(way):
        block = dot(table[:, LOCAL:], pick_near[way])
        for face in range(6):
            store_rows(nbr_near, face, oriented(block[:, face * PEER : face * PEER + PEER], turn_out[way, face]))

    def advance(turn, top_later=False):
        depth = K if top_later else NBR
        if not top_later:
            local_sums(turn)
        receive(turn, top_later)
        far_side = 1 - near_side
        near_part(far_side)
        if top_later:

            @pl.when(space >= 0)
            def _():
                own_out[far_side] = own_out[far_side] + apply(lhs_node, nbr_near, 0, NBR)

            take_top(turn, True)

        @pl.when(slab >= 0)
        def _():
            if top_later:
                late = apply(lhs_node, nbr_far, NBR, K)
                own_out[0] = own_out[0] + late[:, :PEER]
                own_out[1] = own_out[1] + late[:, PEER:]
                send_one(turn + 1, far_side, own_out[far_side])
            else:
                send_one(turn + 1, far_side, own_out[far_side] + apply(lhs_node, nbr_near, 0, NBR))

        update(turn, depth)

        @pl.when(space >= 0)
        def _():
            near_part(near_side)

        @pl.when(slab >= 0)
        def _():
            send_one(turn + 1, near_side, own_out[near_side] + apply(lhs_node, nbr_near, 0, NBR))

    advance(1, True)

    @pl.loop(2, ROUNDS - 1)
    def _(turn):
        advance(turn)

    lhs_time[:E, :] = dot(by_time[...], lhs_node[:E, :]).astype(BF16)
    lhs_time[E:, :] = dot(by_time[...], lhs_node[E:, :]).astype(BF16)
    high, low = halves(const_node[...])
    const_time[...] = dot(by_time[...], high) + dot(by_time[...], low)
    own[...] = local_part(ROUNDS - 1, lhs_time, const_time)
    take_top(ROUNDS - 1)
    own[...] += apply(lhs_time, nbr, NBR, K)
    receive(ROUNDS - 1)
    remote_part(pick, LOCAL, turn_rows)

    @pl.when(slab >= 0)
    def _():
        out[0] = own[...] + apply(lhs_time, nbr_far, 0, NBR)

    for copy in space_copies(ROUNDS - 1) + far_copies + [relay(0), relay(1)]:
        copy.wait_send()

    @pl.when(slab < n_slab - 1)
    def _():
        top_copy(ROUNDS - 1).wait_send()


def body(n_space, n_slab, source, initial, inverse, lift, lift_time, links, orient, exports, counts):
    hbm = pl.BlockSpec(memory_space=pltpu.HBM)
    arrays = (source, initial, inverse, lift, lift_time.T, links, orient, exports.reshape(1, E))
    arrays = [pltpu.with_memory_space_constraint(array, pltpu.HBM) for array in arrays]
    vmem = pltpu.VMEM
    dma = pltpu.SemaphoreType.DMA
    state = pl.pallas_call(
        functools.partial(kernel, n_space, n_slab),
        name="window",
        out_shape=jax.ShapeDtypeStruct((1, 256, E), F32),
        in_specs=[hbm] * 8,
        out_specs=pl.BlockSpec(memory_space=pltpu.VMEM),
        scratch_shapes=[
            vmem((256, E), F32),
            vmem((64, E), F32),
            vmem((256, 256), F32),
            vmem((256, 384), F32),
            vmem((64, 256), F32),
            vmem((6, E), jnp.int32),
            vmem((6, E), jnp.int32),
            vmem((1, E), jnp.int32),
            vmem((TABLE, LOCAL), BF16),
            vmem((2, 2 * PEER, 6 * PEER), BF16),
            vmem((128, TABLE), BF16),
            vmem((K, E), BF16),
            vmem((K, E), BF16),
            vmem((512, K), BF16),
            vmem((512, K), BF16),
            vmem((512, 256), BF16),
            vmem((256, E), F32),
            vmem((256, E), F32),
            vmem((256, 256), BF16),
            vmem((256, 256), BF16),
            vmem((256, E), F32),
            vmem((2, 256, PEER), F32),
            vmem((2, 8, PEER), jnp.int32),
            vmem((NBR, PEER), BF16),
            vmem((256, 512), F32),
            vmem((512, K), BF16),
            vmem((16, LOCAL), jnp.int32),
            vmem((6, 8, E), jnp.int32),
            vmem((2, 6, 8, PEER), jnp.int32),
            vmem((32, E), F32),
            vmem((E, E), BF16),
            vmem((64, 8, E), F32),
            vmem((2, 256, 128), F32),
            vmem((ROUNDS, 2, 64, PEER), F32),
            vmem((ROUNDS, 2, 64, PEER), F32),
            vmem((ROUNDS, 64, E), F32),
            vmem((ROUNDS, 64, E), F32),
            vmem((2, 24, PEER), F32),
            vmem((2, 24, PEER), F32),
            vmem((2, 64, PEER), F32),
            vmem((4 * PEER, LOCAL), BF16),
            vmem((128, 4 * PEER), BF16),
            vmem((6, 8, E), jnp.int32),
            vmem((2, 64, PEER), F32),
            dma((8,)),
            dma((2,)),
            dma((ROUNDS, 2)),
            dma,
            dma((ROUNDS,)),
            dma((2, 2)),
            dma((2, 2)),
        ],
        compiler_params=pltpu.CompilerParams(
            collective_id=0, has_side_effects=True, vmem_limit_bytes=48 * 1024 * 1024
        ),
    )(*arrays)
    live = jnp.arange(E, dtype=jnp.int32) < counts[0]
    return jnp.where(live[None, None, :], state, 0.0)


def solution(mesh):
    return jax.shard_map(
        functools.partial(body, mesh.shape["space"], mesh.shape["slab"]),
        mesh=mesh,
        in_specs=(
            P("slab", None, "space"),
            P(None, "space"),
            P(),
            P(),
            P(),
            P(None, "space"),
            P(None, "space"),
            P("space"),
            P("space"),
        ),
        out_specs=P("slab", None, "space"),
        check_vma=False,
    )
```
